32 devices in a mesh: groups: 2 (over y), seq: 4 (over z), head: 2 (over x), sub: 2 (over core).
Axes of the slice: x: 2, y: 2, z: 4, core: 2. Of those that a mesh axis runs over, the one named last changes fastest.
Arguments:
- queries: bfloat16 [32, 64, 8192], P(('groups', 'seq'), None, 'head'), parts along dimension 0, may hold values from -6 to 6
- new_kv: bfloat16 [32, 64, 2, 1024], P(('groups', 'seq'), None, None, 'head'), parts along dimension 0, may hold values from -6 to 6
- kv_pages: bfloat16 [336, 2, 128, 1024], P(('groups', 'seq', 'sub'), None, None, 'head'), parts along dimension 0, may hold values from -6 to 6
- page_table: int32 [32, 16], P('groups'), parts along dimension 0, may hold values from -1 to 167, as said below
- cached_len: int32 [32], P('groups'), parts along dimension 0, may hold values from 1 to 2048, as said below
- is_prefill: int32 [32], P('groups'), parts along dimension 0, may hold values from 0 to 1, as said below
Outputs:
- attended: bfloat16 [32, 64, 8192], P(('groups', 'seq'), None, 'head'), parts along dimension 0
The draws below stay inside these ranges and needn't reach their ends.
There are 2 independent parts, one for each index of `groups`. The reference program is written for one: setup_inputs(seed, part) draws one part's arguments, and reference() takes and returns one part's arrays. A program takes and returns all parts, laid end to end along the dimension named above; each array names one. Nothing has to cross between parts.
Inputs may be any that keep to these rules, and one draw needn't show every extreme that they name: `page_table`: entry [s, p] is the page number of page p of sequence s for p < ceil(cached_len[s] / 128) and -1 after; page number q lies on owner q // 21 (owner index = seq index * 2 + sub index) in its slot q % 21. Listing the pages of all sequences in order of sequence and page as t = 0, 1, ..., page t has owner (t + c) % 8 and slot (t + c) // 8 for one drawn c. No owner holds more than 8 page of the 4 sequences of one seq shard, and some owner holds exactly 8. `cached_len`: A decode sequence has 1 to 4 cache pages, a prefill sequence 8 to 16; all 4 sequences of one drawn seq shard are prefill sequences with 16 pages. `is_prefill`: exactly 8 sequences are prefill sequences.
All inputs are finite; a program needn't handle non-finite values.
Results may differ from the reference program's by a relative error of at most 0.014.
Values may be sent and summed in bfloat16 or wider, within the bound.
A program may use at most 64 MiB of HBM per device.

```python
import jax
import jax.numpy as jnp
from jax import lax

HQ = 64
KVH = 8
HD = 128
PAGE = 128
MAXP = 16
DEC_MAXP = 4
QROWS = 64
SEQ_DEV = 4
SEQS = 16
PREFILL = 8
OWNERS = 8
PAGES_DEV = 21


def page_layout(key):
    heavy_key = jax.random.fold_in(key, 101)
    order_key = jax.random.fold_in(key, 102)
    long_key = jax.random.fold_in(key, 103)
    short_key = jax.random.fold_in(key, 104)
    tail_key = jax.random.fold_in(key, 105)
    rotate_key = jax.random.fold_in(key, 106)
    shard_total = SEQS // SEQ_DEV
    heavy = jax.random.randint(heavy_key, (), 0, shard_total)
    seq_ids = jnp.arange(SEQS, dtype=jnp.int32)
    in_heavy = seq_ids // SEQ_DEV == heavy
    shuffled = jax.random.permutation(order_key, SEQS).astype(jnp.int32)
    keyed = jnp.where(in_heavy, -1, shuffled)
    standing = jnp.sum((keyed[None, :] < keyed[:, None]).astype(jnp.int32), axis=1)
    prefill = standing < PREFILL
    long_pages = jax.random.randint(long_key, (SEQS,), MAXP // 2, MAXP + 1)
    short_pages = jax.random.randint(short_key, (SEQS,), 1, DEC_MAXP + 1)
    page_total = jnp.where(in_heavy, MAXP, jnp.where(prefill, long_pages, short_pages)).astype(jnp.int32)
    cached = (page_total - 1) * PAGE + jax.random.randint(tail_key, (SEQS,), 1, PAGE + 1)
    first_page = jnp.cumsum(page_total) - page_total
    rotation = jax.random.randint(rotate_key, (), 0, OWNERS)
    page_ids = jnp.arange(MAXP, dtype=jnp.int32)
    linear = first_page[:, None] + page_ids[None, :] + rotation
    number = linear % OWNERS * PAGES_DEV + linear // OWNERS
    table_rows = jnp.where(page_ids[None, :] < page_total[:, None], number, -1)
    return (table_rows.astype(jnp.int32), cached.astype(jnp.int32), prefill.astype(jnp.int32))


def draw_page_table(key, part):
    return page_layout(key)[0]


def draw_cached_len(key, part):
    return page_layout(key)[1]


def draw_is_prefill(key, part):
    return page_layout(key)[2]


def draw_queries(key, part):
    shape = (SEQS, QROWS, HQ * HD)
    values = jnp.clip(jax.random.normal(jax.random.fold_in(key, 11), shape, jnp.float32), -5.0, 5.0)
    return values.astype(jnp.bfloat16)


def draw_kv_pages(key, part):
    shape = (PAGES_DEV * OWNERS, 2, PAGE, KVH * HD)
    values = jnp.clip(jax.random.normal(jax.random.fold_in(key, 12), shape, jnp.float32), -5.0, 5.0)
    return values.astype(jnp.bfloat16)


def block_levels(stream_key, extent, pieces, least, largest):
    loudness, own = 1.0, jax.random.fold_in(stream_key, 6)
    for dim, blocks in pieces:
        steps = jnp.exp(jax.random.uniform(jax.random.fold_in(own, dim), (blocks,), jnp.float32, least / len(pieces), largest / len(pieces)))
        loudness = loudness * jnp.repeat(steps, extent[dim] // blocks).reshape([-1 if axis == dim else 1 for axis in range(len(extent))])
    return loudness


def normal_values(rng, shape, scale, bound, pieces=(), kind=jnp.bfloat16):
    level = block_levels(rng, shape, pieces, -0.22, 0.18) if pieces else 1.0
    values = jax.random.normal(rng, shape, jnp.float32) * scale * level
    return jnp.minimum(jnp.maximum(values, -bound), bound).astype(kind)


def setup_inputs(seed: int = 0, part: int = 0) -> dict:
    splits = jax.random.split(jax.random.key(seed), 7)
    own_keys = jax.random.split(jax.random.fold_in(splits[6], part), 7)
    return {
        "queries": draw_queries(jax.random.fold_in(jax.random.fold_in(splits[6], part), 71), part),
        "new_kv": normal_values(own_keys[1], (SEQS, QROWS, 2, KVH * HD), 1.0, 6.0, ((0, 4), (3, 2))),
        "kv_pages": draw_kv_pages(jax.random.fold_in(jax.random.fold_in(splits[6], part), 71), part),
        "page_table": draw_page_table(jax.random.fold_in(jax.random.fold_in(splits[6], part), 71), part),
        "cached_len": draw_cached_len(jax.random.fold_in(jax.random.fold_in(splits[6], part), 71), part),
        "is_prefill": draw_is_prefill(jax.random.fold_in(jax.random.fold_in(splits[6], part), 71), part),
    }


NEG_FILL = -1e30


def reference(queries, new_kv, kv_pages, page_table, cached_len, is_prefill):
    group_size = HQ // KVH
    score_scale = HD ** -0.5
    positions = jnp.arange(MAXP * PAGE, dtype=jnp.int32)
    row_ids = jnp.arange(QROWS, dtype=jnp.int32)
    causal = row_ids[None, :] <= row_ids[:, None]

    def one_sequence(inputs):
        query_rows, fresh_rows, table_row, length, flag = inputs
        fetched = jnp.take(kv_pages, jnp.maximum(table_row, 0).astype(jnp.int32), axis=0)
        cache_keys = fetched[:, 0].reshape(MAXP * PAGE, KVH, HD).astype(jnp.float32)
        cache_values = fetched[:, 1].reshape(MAXP * PAGE, KVH, HD).astype(jnp.float32)
        cache_valid = positions < length
        live_row = (flag == 1) | (row_ids == 0)
        query_heads = query_rows.reshape(QROWS, KVH, group_size, HD).astype(jnp.float32)
        fresh_keys = fresh_rows[:, 0].reshape(QROWS, KVH, HD).astype(jnp.float32)
        fresh_values = fresh_rows[:, 1].reshape(QROWS, KVH, HD).astype(jnp.float32)
        fresh_valid = causal & live_row[:, None]
        cache_scores = jnp.einsum("rkgd,nkd->kgrn", query_heads, cache_keys) * score_scale
        fresh_scores = jnp.einsum("rkgd,jkd->kgrj", query_heads, fresh_keys) * score_scale
        cache_mask = cache_valid[None, None, None, :]
        fresh_mask = fresh_valid[None, None, :, :]
        peak = jnp.maximum(jnp.max(jnp.where(cache_mask, cache_scores, NEG_FILL), axis=-1),
                           jnp.max(jnp.where(fresh_mask, fresh_scores, NEG_FILL), axis=-1))
        cache_weights = jnp.where(cache_mask, jnp.exp(cache_scores - peak[..., None]), 0.0)
        fresh_weights = jnp.where(fresh_mask, jnp.exp(fresh_scores - peak[..., None]), 0.0)
        weight_sum = jnp.sum(cache_weights, axis=-1) + jnp.sum(fresh_weights, axis=-1)
        cache_rounded = lax.optimization_barrier(cache_weights.astype(jnp.bfloat16)).astype(jnp.float32)
        fresh_rounded = lax.optimization_barrier(fresh_weights.astype(jnp.bfloat16)).astype(jnp.float32)
        numerator = jnp.einsum("kgrn,nkd->kgrd", cache_rounded, cache_values)
        numerator = numerator + jnp.einsum("kgrj,jkd->kgrd", fresh_rounded, fresh_values)
        unused_rows = 1.0 - live_row.astype(jnp.float32)
        attended = numerator / (weight_sum + unused_rows[None, None, :])[..., None]
        attended = jnp.where(live_row[None, None, :, None], attended, 0.0)
        return jnp.transpose(attended, (2, 0, 1, 3)).reshape(QROWS, HQ * HD).astype(jnp.bfloat16)

    return lax.map(one_sequence, (queries, new_kv, page_table, cached_len, is_prefill))
```

```python
import functools

import jax
import jax.numpy as jnp
from jax import lax
from jax.experimental import pallas as pl
from jax.experimental.pallas import tpu as pltpu
from jax.sharding import PartitionSpec as P

HD = 128
PAGE = 128


NEG_FILL = -1e30


def partial_softmax(
    query_heads, cache_keys, cache_values, cache_valid, fresh_keys, fresh_values, fresh_valid
):
    score_scale = HD ** (-0.5)
    cache_scores = (
        jnp.einsum("rkgd,nkd->kgrn", query_heads, cache_keys, preferred_element_type=jnp.float32)
        * score_scale
    )
    fresh_scores = (
        jnp.einsum("rkgd,jkd->kgrj", query_heads, fresh_keys, preferred_element_type=jnp.float32)
        * score_scale
    )
    cache_mask = cache_valid[None, None, None, :]
    fresh_mask = fresh_valid[None, None, :, :]
    peak = jnp.maximum(
        jnp.max(jnp.where(cache_mask, cache_scores, NEG_FILL), axis=-1),
        jnp.max(jnp.where(fresh_mask, fresh_scores, NEG_FILL), axis=-1),
    )
    cache_weights = jnp.where(cache_mask, jnp.exp(cache_scores - peak[..., None]), 0.0)
    fresh_weights = jnp.where(fresh_mask, jnp.exp(fresh_scores - peak[..., None]), 0.0)
    weight_sum = jnp.sum(cache_weights, axis=-1) + jnp.sum(fresh_weights, axis=-1)
    numerator = jnp.einsum(
        "kgrn,nkd->kgrd",
        cache_weights.astype(jnp.bfloat16),
        cache_values,
        preferred_element_type=jnp.float32,
    )
    numerator = numerator + jnp.einsum(
        "kgrj,jkd->kgrd",
        fresh_weights.astype(jnp.bfloat16),
        fresh_values,
        preferred_element_type=jnp.float32,
    )
    return (peak, weight_sum, numerator)


def attend_all(
    query_block, fresh_block, received, fetch_index, page_here, lengths, live_rows, causal, fresh_on
):
    kv_width = received.shape[-1]
    heads_kv = kv_width // HD
    row_count = query_block.shape[1]
    group_size = query_block.shape[2] // kv_width
    page_count = fetch_index.shape[1]
    positions = jnp.arange(page_count * PAGE, dtype=jnp.int32)

    def one_sequence(inputs):
        query_rows, fresh_rows, index_row, here_row, length, live_row = inputs
        fetched = jnp.take(received, index_row, axis=0)
        cache_keys = fetched[:, 0].reshape(page_count * PAGE, heads_kv, HD)
        cache_values = fetched[:, 1].reshape(page_count * PAGE, heads_kv, HD)
        page_mask = jnp.broadcast_to(here_row[:, None], (page_count, PAGE)).reshape(
            page_count * PAGE
        )
        cache_valid = page_mask & (positions < length)
        query_heads = query_rows.reshape(row_count, heads_kv, group_size, HD)
        fresh_keys = fresh_rows[:, 0].reshape(row_count, heads_kv, HD)
        fresh_values = fresh_rows[:, 1].reshape(row_count, heads_kv, HD)
        fresh_valid = causal & live_row[:, None] & fresh_on
        return partial_softmax(
            query_heads,
            cache_keys,
            cache_values,
            cache_valid,
            fresh_keys,
            fresh_values,
            fresh_valid,
        )

    return lax.map(
        one_sequence, (query_block, fresh_block, fetch_index, page_here, lengths, live_rows)
    )


def finish(weight_sum, numerator, live_rows):
    unused_rows = 1.0 - live_rows.astype(jnp.float32)
    attended = numerator / (weight_sum + unused_rows[:, None, None, :])[..., None]
    attended = jnp.where(live_rows[:, None, None, :, None], attended, 0.0)
    seq_dev, heads_kv, group_size, row_count, head_dim = attended.shape
    return (
        jnp.transpose(attended, (0, 3, 1, 2, 4))
        .reshape(seq_dev, row_count, heads_kv * group_size * head_dim)
        .astype(jnp.bfloat16)
    )


def exchange_pages(queries, new_kv, kv_pages, page_table, cached_len, is_prefill):
    seq_shards = lax.axis_size("seq")
    sub_count = lax.axis_size("sub")
    owners = seq_shards * sub_count
    seq_index = lax.axis_index("seq")
    core_index = lax.axis_index("sub")
    owner_self = seq_index * sub_count + core_index
    seq_dev, row_count, query_width = queries.shape
    pages_dev = kv_pages.shape[0]
    kv_width = kv_pages.shape[3]
    page_count = page_table.shape[1]
    entries = seq_dev * page_count
    capacity = (entries + owners - 1) // owners
    table_rows = page_table.reshape(seq_shards, entries)
    holder = jnp.where(table_rows >= 0, table_rows // pages_dev, -1)
    slot_of = jnp.where(table_rows >= 0, table_rows % pages_dev, 0)
    owned_here = holder == owner_self
    rank_among = jnp.cumsum(owned_here.astype(jnp.int32), axis=1) - 1
    picked = owned_here[:, :, None] & (
        rank_among[:, :, None] == jnp.arange(capacity, dtype=jnp.int32)[None, None, :]
    )
    send_slots = jnp.sum(jnp.where(picked, slot_of[:, :, None], 0), axis=1).reshape(
        seq_shards * capacity
    )
    first_seq = seq_index * seq_dev
    my_table = lax.dynamic_slice_in_dim(page_table, first_seq, seq_dev, 0)
    my_lengths = lax.dynamic_slice_in_dim(cached_len, first_seq, seq_dev, 0)
    my_flags = lax.dynamic_slice_in_dim(is_prefill, first_seq, seq_dev, 0)
    flat_table = my_table.reshape(entries)
    my_holder = jnp.where(flat_table >= 0, flat_table // pages_dev, -1)
    entry_order = jnp.arange(entries, dtype=jnp.int32)
    earlier = (my_holder[:, None] == my_holder[None, :]) & (
        entry_order[None, :] < entry_order[:, None]
    )
    my_rank = jnp.sum(earlier.astype(jnp.int32), axis=1)
    row_ids = jnp.arange(row_count, dtype=jnp.int32)
    live_rows = (my_flags[:, None] == 1) | (row_ids[None, :] == 0)
    causal = row_ids[None, :] <= row_ids[:, None]
    part_width = kv_width // sub_count
    split_pages = kv_pages.reshape(pages_dev, 2, PAGE, sub_count, part_width)
    chosen = jnp.take(split_pages, send_slots, axis=0).reshape(
        seq_shards, capacity, 2, PAGE, sub_count, part_width
    )
    outgoing = jnp.moveaxis(chosen, 4, 1).reshape(owners, capacity, 2, PAGE, part_width)
    received = lax.all_to_all(
        outgoing, ("seq", "sub"), split_axis=0, concat_axis=0, tiled=True
    ).reshape(owners * capacity, 2, PAGE, part_width)
    present = flat_table >= 0
    fetch_index = jnp.where(present, my_holder * capacity + my_rank, 0)
    query_part = query_width // sub_count
    my_queries = lax.dynamic_slice_in_dim(queries, core_index * query_part, query_part, 2)
    my_fresh = lax.dynamic_slice_in_dim(new_kv, core_index * part_width, part_width, 3)
    peak, weight_sum, numerator = attend_all(
        my_queries,
        my_fresh,
        received,
        fetch_index.reshape(seq_dev, page_count),
        present.reshape(seq_dev, page_count),
        my_lengths,
        live_rows,
        causal,
        core_index >= 0,
    )
    own_heads = finish(weight_sum, numerator, live_rows)
    return lax.all_gather(own_heads, "sub", axis=2, tiled=True)


MESH = pl.DeviceIdType.MESH
SCALE = HD ** (-0.5)


def greet(z, n):
    has_left, has_right = z > 0, z < n - 1
    barrier = pltpu.get_barrier_semaphore()

    @pl.when(has_left)
    def _():
        pl.semaphore_signal(barrier, inc=1, device_id={"seq": z - 1}, device_id_type=MESH)

    @pl.when(has_right)
    def _():
        pl.semaphore_signal(barrier, inc=1, device_id={"seq": z + 1}, device_id_type=MESH)

    pl.semaphore_wait(barrier, has_left.astype(jnp.int32) + has_right.astype(jnp.int32))
    return has_left, has_right


def remote(src, dst, send, recv, z):
    return pltpu.make_async_remote_copy(
        src_ref=src, dst_ref=dst, send_sem=send, recv_sem=recv,
        device_id={"seq": z}, device_id_type=MESH,
    )


def gather_queries_kernel(n, chunks, own, out, rin, rout, lin, lout, rs, rr, ls, lr):
    z = lax.axis_index("seq")
    has_left, has_right = greet(z, n)
    for c, (start, size) in enumerate(chunks):
        rows = pl.ds(start, size)
        right = remote(rout.at[rows], rin.at[rows], rs.at[c], rr.at[c], z + 1)
        left = remote(lout.at[rows], lin.at[rows], ls.at[c], lr.at[c], z - 1)

        @pl.when(has_left)
        def _():
            right.wait_recv()
            rout[rows] = own[rows] + rin[rows]

        @pl.when(jnp.logical_not(has_left))
        def _():
            rout[rows] = own[rows]

        @pl.when(has_right)
        def _():
            right.start()
            left.wait_recv()
            lout[rows] = own[rows] + lin[rows]
            out[rows] = rout[rows] + lin[rows]

        @pl.when(jnp.logical_not(has_right))
        def _():
            lout[rows] = own[rows]
            out[rows] = rout[rows]

        @pl.when(has_left)
        def _():
            left.start()

    for c, (start, size) in enumerate(chunks):
        rows = pl.ds(start, size)

        @pl.when(has_right)
        def _():
            remote(rout.at[rows], rin.at[rows], rs.at[c], rr.at[c], z + 1).wait_send()

        @pl.when(has_left)
        def _():
            remote(lout.at[rows], lin.at[rows], ls.at[c], lr.at[c], z - 1).wait_send()


def gather_queries(own, n, row_count):
    total, width = own.shape
    chunks = []
    start = 0
    while start < total:
        size = min(row_count // 2, total - start)
        chunks.append((start, size))
        start += size
    count = len(chunks)
    buffer = pltpu.VMEM(own.shape, own.dtype)
    return pl.pallas_call(
        functools.partial(gather_queries_kernel, n, chunks),
        out_shape=jax.ShapeDtypeStruct(own.shape, own.dtype),
        in_specs=[pl.BlockSpec(memory_space=pltpu.VMEM)],
        out_specs=pl.BlockSpec(memory_space=pltpu.VMEM),
        scratch_shapes=[buffer] * 4 + [pltpu.SemaphoreType.DMA((count,))] * 4,
        compiler_params=pltpu.CompilerParams(collective_id=0, has_side_effects=True),
        name="gather_queries",
    )(own)


def merge(o1, e1, o2, e2):
    top = jnp.maximum(e1, e2)
    w1, w2 = jnp.exp(e1 - top), jnp.exp(e2 - top)
    total = w1 + w2
    inv = 1.0 / total
    return o1 * (w1 * inv) + o2 * (w2 * inv), top + jnp.log(total)


def reduce_outputs_kernel(
    n, parts, heads, o, e, od, ed, out, oute, outd, outed, *scratch
):
    rino, rouo, lino, louo, rine, roue, line, loue = scratch[:8]
    drino, drouo, dlino, dlouo, drine, droue, dline, dloue = scratch[8:16]
    rs, rr, ls, lr, res, rer, les, ler = scratch[16:]
    z = lax.axis_index("seq")
    has_left, has_right = greet(z, n)
    views = []
    for c in range(parts + 1):
        if c == 0:
            refs = (od, ed, outd, outed, drino, drouo, dlino, dlouo, drine, droue, dline, dloue)
            views.append(refs)
        else:
            refs = (o, e, out, oute, rino, rouo, lino, louo, rine, roue, line, loue)
            views.append(tuple(r.at[c - 1] for r in refs))

    def copies(c):
        _, _, _, _, ri, ro, li, lo, rei, reo, lei, leo = views[c]
        to_right = (
            remote(ro, ri, rs.at[c], rr.at[c], z + 1),
            remote(reo, rei, res.at[c], rer.at[c], z + 1),
        )
        to_left = (
            remote(lo, li, ls.at[c], lr.at[c], z - 1),
            remote(leo, lei, les.at[c], ler.at[c], z - 1),
        )
        return to_right, to_left

    def join(o1, e1, o2, e2, oo, eo):
        for k in range(heads):
            rows = pl.ds(k * HD, HD)
            joined, stat = merge(
                o1[rows].astype(jnp.float32), e1[pl.ds(k, 1)], o2[rows].astype(jnp.float32), e2[pl.ds(k, 1)]
            )
            oo[rows] = joined.astype(oo.dtype)
            eo[pl.ds(k, 1)] = stat

    for c in range(parts + 1):
        ov, ev, outv, outev, ri, ro, li, lo, rei, reo, lei, leo = views[c]
        to_right, to_left = copies(c)

        @pl.when(has_left)
        def _():
            for x in to_right:
                x.wait_recv()
            join(ov, ev, ri, rei, ro, reo)

        @pl.when(jnp.logical_not(has_left))
        def _():
            ro[...] = ov[...]
            reo[...] = ev[...]

        @pl.when(has_right)
        def _():
            for x in to_right:
                x.start()
            for x in to_left:
                x.wait_recv()
            join(ov, ev, li, lei, lo, leo)

        @pl.when(jnp.logical_not(has_right))
        def _():
            lo[...] = ov[...]
            leo[...] = ev[...]

        @pl.when(has_left)
        def _():
            for x in to_left:
                x.start()

        @pl.when(has_right)
        def _():
            join(ro, reo, li, lei, outv, outev)

        @pl.when(jnp.logical_not(has_right))
        def _():
            outv[...] = ro[...]
            outev[...] = reo[...]

    for c in range(parts + 1):
        to_right, to_left = copies(c)

        @pl.when(has_right)
        def _():
            for x in to_right:
                x.wait_send()

        @pl.when(has_left)
        def _():
            for x in to_left:
                x.wait_send()


def reduce_outputs(o, e, od, ed, n):
    parts, heads = e.shape[:2]
    shapes = [jax.ShapeDtypeStruct(x.shape, x.dtype) for x in (o, e, od, ed)]
    big = [pltpu.VMEM(o.shape, o.dtype)] * 4 + [pltpu.VMEM(e.shape, e.dtype)] * 4
    small = [pltpu.VMEM(od.shape, od.dtype)] * 4 + [pltpu.VMEM(ed.shape, ed.dtype)] * 4
    return pl.pallas_call(
        functools.partial(reduce_outputs_kernel, n, parts, heads),
        out_shape=shapes,
        in_specs=[pl.BlockSpec(memory_space=pltpu.VMEM)] * 4,
        out_specs=[pl.BlockSpec(memory_space=pltpu.VMEM)] * 4,
        scratch_shapes=big + small + [pltpu.SemaphoreType.DMA((parts + 1,))] * 8,
        compiler_params=pltpu.CompilerParams(collective_id=1, has_side_effects=True),
        name="reduce_outputs",
    )(o, e, od, ed)


def stacked_heads(rows, k, group_size):
    return jnp.concatenate(
        [rows[:, (k * group_size + g) * HD : (k * group_size + g + 1) * HD] for g in range(group_size)], axis=0
    )


def scores_of(keys, query):
    return (
        lax.dot_general(keys, query, (((1,), (1,)), ((), ())), preferred_element_type=jnp.float32) * SCALE
    )


def partial_outputs(query, blocks):
    scored = [jnp.where(mask, scores_of(keys, query), NEG_FILL) for keys, _, mask in blocks]
    peak = functools.reduce(jnp.maximum, [jnp.max(s, axis=0, keepdims=True) for s in scored])
    acc, total = None, None
    for s, (_, values, mask) in zip(scored, blocks):
        weights = jnp.where(mask, jnp.exp(s - peak), 0.0)
        part = jnp.sum(weights, axis=0, keepdims=True)
        prod = lax.dot_general(
            values, weights.astype(jnp.bfloat16), (((0,), (0,)), ((), ())), preferred_element_type=jnp.float32
        )
        acc = prod if acc is None else acc + prod
        total = part if total is None else total + part
    empty = total == 0.0
    total = jnp.where(empty, 1.0, total)
    return acc * (1.0 / total), jnp.where(empty, NEG_FILL, peak + jnp.log(total))


def prefill_kernel(most, heads, group_size, pages, valid, home, local, q_ref, *refs):
    page_refs, (fk_ref, fv_ref, o_ref, e_ref) = refs[:most], refs[most:]
    j = pl.program_id(0)
    rows = q_ref.shape[0]
    lanes = group_size * rows
    key_id = lax.broadcasted_iota(jnp.int32, (PAGE, 1), 0)
    fresh_id = lax.broadcasted_iota(jnp.int32, (rows, lanes), 0)
    lane_row = lax.broadcasted_iota(jnp.int32, (rows, lanes), 1) % rows
    for k in range(heads):
        cols = slice(k * HD, (k + 1) * HD)
        query = stacked_heads(q_ref, k, group_size)
        blocks = [
            (ref[0, 0, :, cols], ref[0, 1, :, cols], key_id < valid[j, i]) for i, ref in enumerate(page_refs)
        ]
        fresh_mask = (fresh_id <= lane_row) & (home[j] == 1)
        blocks.append((fk_ref[0, :, cols], fv_ref[0, :, cols], fresh_mask))
        o, e = partial_outputs(query, blocks)
        o_ref[0, cols, :] = o.astype(o_ref.dtype)
        e_ref[0, k : k + 1, :] = e


def decode_kernel(most, heads, group_size, seqs, pages, valid, home, local, seq, q_ref, *refs):
    page_refs, (fk_ref, fv_ref, o_ref, e_ref) = refs[:most], refs[most:]
    j = pl.program_id(0)
    lanes = group_size * seqs
    fresh_rows = 16
    key_id = lax.broadcasted_iota(jnp.int32, (PAGE, 1), 0)
    fresh_id = lax.broadcasted_iota(jnp.int32, (fresh_rows, 1), 0)
    mine = lax.broadcasted_iota(jnp.int32, (1, lanes), 1) % seqs == seq[j]

    @pl.when(j == 0)
    def _():
        o_ref[...] = jnp.zeros_like(o_ref)
        e_ref[...] = jnp.full_like(e_ref, NEG_FILL)

    for k in range(heads):
        cols = slice(k * HD, (k + 1) * HD)
        query = stacked_heads(q_ref, k, group_size)
        blocks = [
            (ref[0, 0, :, cols], ref[0, 1, :, cols], key_id < valid[j, i]) for i, ref in enumerate(page_refs)
        ]
        fresh_mask = fresh_id < home[j]
        blocks.append((fk_ref[0, :fresh_rows, cols], fv_ref[0, :fresh_rows, cols], fresh_mask))
        o, e = partial_outputs(query, blocks)
        o_ref[cols, :] = jnp.where(mine, o, o_ref[cols, :].astype(jnp.float32)).astype(o_ref.dtype)
        e_ref[k : k + 1, :] = jnp.where(mine, e, e_ref[k : k + 1, :])


def finish_kernel(heads, group_size, seqs, slot, flag, first, o_ref, od_ref, out_ref):
    i = pl.program_id(0)
    rows = out_ref.shape[1]

    @pl.when(flag[i] == 1)
    def _():
        for k in range(heads):
            turned = o_ref[0, k * HD : (k + 1) * HD, :].astype(jnp.float32).T.astype(out_ref.dtype)
            for g in range(group_size):
                h = k * group_size + g
                out_ref[0, :, h * HD : (h + 1) * HD] = turned[g * rows : (g + 1) * rows]

    @pl.when(flag[i] != 1)
    def _():
        top = lax.broadcasted_iota(jnp.int32, (rows, 1), 0) == 0
        pick = lax.broadcasted_iota(jnp.int32, (seqs, 1), 0) == first[0] + i
        for k in range(heads):
            turned = od_ref[k * HD : (k + 1) * HD, :].astype(jnp.float32).T
            for g in range(group_size):
                h = k * group_size + g
                line = jnp.sum(jnp.where(pick, turned[g * seqs : (g + 1) * seqs], 0.0), axis=0, keepdims=True)
                out_ref[0, :, h * HD : (h + 1) * HD] = jnp.where(top, line, 0.0).astype(out_ref.dtype)


def move_queries(queries, new_kv, kv_pages, page_table, cached_len, is_prefill):
    n = lax.axis_size("seq")
    sub_count = lax.axis_size("sub")
    z = lax.axis_index("seq")
    core = lax.axis_index("sub")
    seq_dev, row_count, query_width = queries.shape
    pages_dev, kv_width = kv_pages.shape[0], kv_pages.shape[3]
    seqs, page_count = page_table.shape
    owners = n * sub_count
    most = sub_count * (page_count // owners)
    slots = seqs // 2
    group_size = query_width // kv_width
    part_width, query_part = kv_width // sub_count, query_width // sub_count
    heads = part_width // HD

    other = (core + 1) % sub_count
    away = lax.dynamic_slice_in_dim(kv_pages, other * part_width, part_width, 3)
    here = lax.dynamic_slice_in_dim(kv_pages, core * part_width, part_width, 3)
    came = lax.ppermute(away, "sub", [(c, (c + 1) % sub_count) for c in range(sub_count)])
    pool = jnp.concatenate([here, came], axis=0)

    seq_ids = jnp.arange(seqs, dtype=jnp.int32)
    owner = page_table // pages_dev
    mine = (page_table >= 0) & (owner // sub_count == z)
    index = page_table % pages_dev + jnp.where(owner % sub_count == core, 0, pages_dev)
    rank = jnp.cumsum(mine.astype(jnp.int32), axis=1) - 1
    picked = mine[:, :, None] & (rank[:, :, None] == jnp.arange(most, dtype=jnp.int32))
    tokens = jnp.clip(cached_len[:, None] - PAGE * jnp.arange(page_count, dtype=jnp.int32), 0, PAGE)
    page_rows = jnp.sum(jnp.where(picked, index[:, :, None], 0), axis=1)
    valid_rows = jnp.sum(jnp.where(picked, tokens[:, :, None], 0), axis=1)
    flags = is_prefill == 1
    slot_of = jnp.cumsum(flags.astype(jnp.int32)) - 1
    place_of = jnp.cumsum((~flags).astype(jnp.int32)) - 1
    slot_ids = jnp.arange(slots, dtype=jnp.int32)
    slot_seq = jnp.sum(jnp.where(flags & (slot_of == slot_ids[:, None]), seq_ids, 0), axis=1)
    rest_ids = jnp.arange(seqs - slots, dtype=jnp.int32)
    rest_seq = jnp.sum(jnp.where(~flags & (place_of == rest_ids[:, None]), seq_ids, 0), axis=1)

    def tables(which):
        at_home = (which // seq_dev == z).astype(jnp.int32)
        return page_rows[which], valid_rows[which], at_home, jnp.where(at_home == 1, which % seq_dev, 0)

    slot_tables, rest_tables = tables(slot_seq), tables(rest_seq)
    my_queries = lax.dynamic_slice_in_dim(queries, core * query_part, query_part, 2)
    own_slots = jnp.where((slot_tables[2] == 1)[:, None, None], my_queries[slot_tables[3]], 0)
    first_rows = jnp.where(
        (seq_ids // seq_dev == z)[:, None], jnp.tile(my_queries[:, 0], (n, 1)), 0
    )
    own = jnp.concatenate([own_slots.reshape(slots * row_count, query_part), first_rows], axis=0)
    gathered = gather_queries(own.astype(queries.dtype), n, row_count)

    my_fresh = lax.dynamic_slice_in_dim(new_kv, core * part_width, part_width, 3)
    fresh_keys, fresh_values = my_fresh[:, :, 0], my_fresh[:, :, 1]
    lanes = group_size * row_count
    rest_lanes = group_size * seqs

    def page_spec(i):
        return pl.BlockSpec((1, 2, PAGE, part_width), lambda j, pages, *_: (pages[j, i], 0, 0, 0))

    fresh_spec = pl.BlockSpec(
        (1, row_count, part_width), lambda j, pages, valid, home, local, *_: (local[j], 0, 0)
    )
    o, e = pl.pallas_call(
        functools.partial(prefill_kernel, most, heads, group_size),
        grid_spec=pltpu.PrefetchScalarGridSpec(
            num_scalar_prefetch=4,
            grid=(slots,),
            in_specs=[pl.BlockSpec((row_count, query_part), lambda j, *_: (j, 0))]
            + [page_spec(i) for i in range(most)]
            + [fresh_spec] * 2,
            out_specs=[
                pl.BlockSpec((1, part_width, lanes), lambda j, *_: (j, 0, 0)),
                pl.BlockSpec((1, heads, lanes), lambda j, *_: (j, 0, 0)),
            ],
        ),
        out_shape=[
            jax.ShapeDtypeStruct((slots, part_width, lanes), jnp.bfloat16),
            jax.ShapeDtypeStruct((slots, heads, lanes), jnp.float32),
        ],
        name="prefill_attention",
    )(*slot_tables, gathered, *([pool] * most), fresh_keys, fresh_values)
    od, ed = pl.pallas_call(
        functools.partial(decode_kernel, most, heads, group_size, seqs),
        grid_spec=pltpu.PrefetchScalarGridSpec(
            num_scalar_prefetch=5,
            grid=(seqs - slots,),
            in_specs=[pl.BlockSpec((seqs, query_part), lambda j, *_: (slots * row_count // seqs, 0))]
            + [page_spec(i) for i in range(most)]
            + [fresh_spec] * 2,
            out_specs=[
                pl.BlockSpec((part_width, rest_lanes), lambda j, *_: (0, 0)),
                pl.BlockSpec((heads, rest_lanes), lambda j, *_: (0, 0)),
            ],
        ),
        out_shape=[
            jax.ShapeDtypeStruct((part_width, rest_lanes), jnp.bfloat16),
            jax.ShapeDtypeStruct((heads, rest_lanes), jnp.float32),
        ],
        name="decode_attention",
    )(*rest_tables, rest_seq, gathered, *([pool] * most), fresh_keys, fresh_values)
    o, _, od, _ = reduce_outputs(o, e, od, ed, n)

    first_seq = z * seq_dev
    my_flags = lax.dynamic_slice_in_dim(is_prefill, first_seq, seq_dev, 0)
    my_slots = jnp.maximum(lax.dynamic_slice_in_dim(slot_of, first_seq, seq_dev, 0), 0)
    own_heads = pl.pallas_call(
        functools.partial(finish_kernel, heads, group_size, seqs),
        grid_spec=pltpu.PrefetchScalarGridSpec(
            num_scalar_prefetch=3,
            grid=(seq_dev,),
            in_specs=[
                pl.BlockSpec((1, part_width, lanes), lambda i, slot, *_: (slot[i], 0, 0)),
                pl.BlockSpec((part_width, rest_lanes), lambda i, *_: (0, 0)),
            ],
            out_specs=pl.BlockSpec((1, row_count, query_part), lambda i, *_: (i, 0, 0)),
        ),
        out_shape=jax.ShapeDtypeStruct((seq_dev, row_count, query_part), jnp.bfloat16),
        name="finish",
    )(my_slots, my_flags, jnp.reshape(first_seq, (1,)).astype(jnp.int32), o, od)
    return lax.all_gather(own_heads, "sub", axis=2, tiled=True)


def per_device(queries, new_kv, kv_pages, page_table, cached_len, is_prefill):
    owners = lax.axis_size("seq") * lax.axis_size("sub")
    if page_table.shape[1] >= owners:
        return move_queries(queries, new_kv, kv_pages, page_table, cached_len, is_prefill)
    return exchange_pages(queries, new_kv, kv_pages, page_table, cached_len, is_prefill)


def solution(mesh):
    placed = (
        P(("groups", "seq"), None, "head"),
        P(("groups", "seq"), None, None, "head"),
        P(("groups", "seq", "sub"), None, None, "head"),
        P("groups", None),
        P("groups"),
        P("groups"),
    )
    return jax.shard_map(
        per_device,
        mesh=mesh,
        in_specs=placed,
        out_specs=P(("groups", "seq"), None, "head"),
        check_vma=False,
    )
```

```python
import functools

import jax
import jax.numpy as jnp
from jax import lax
from jax.experimental import pallas as pl
from jax.experimental.pallas import tpu as pltpu
from jax.sharding import PartitionSpec as P

HD = 128
PAGE = 128


NEG_FILL = -1e30


def partial_softmax(
    query_heads, cache_keys, cache_values, cache_valid, fresh_keys, fresh_values, fresh_valid
):
    score_scale = HD ** (-0.5)
    cache_scores = (
        jnp.einsum("rkgd,nkd->kgrn", query_heads, cache_keys, preferred_element_type=jnp.float32)
        * score_scale
    )
    fresh_scores = (
        jnp.einsum("rkgd,jkd->kgrj", query_heads, fresh_keys, preferred_element_type=jnp.float32)
        * score_scale
    )
    cache_mask = cache_valid[None, None, None, :]
    fresh_mask = fresh_valid[None, None, :, :]
    peak = jnp.maximum(
        jnp.max(jnp.where(cache_mask, cache_scores, NEG_FILL), axis=-1),
        jnp.max(jnp.where(fresh_mask, fresh_scores, NEG_FILL), axis=-1),
    )
    cache_weights = jnp.where(cache_mask, jnp.exp(cache_scores - peak[..., None]), 0.0)
    fresh_weights = jnp.where(fresh_mask, jnp.exp(fresh_scores - peak[..., None]), 0.0)
    weight_sum = jnp.sum(cache_weights, axis=-1) + jnp.sum(fresh_weights, axis=-1)
    numerator = jnp.einsum(
        "kgrn,nkd->kgrd",
        cache_weights.astype(jnp.bfloat16),
        cache_values,
        preferred_element_type=jnp.float32,
    )
    numerator = numerator + jnp.einsum(
        "kgrj,jkd->kgrd",
        fresh_weights.astype(jnp.bfloat16),
        fresh_values,
        preferred_element_type=jnp.float32,
    )
    return (peak, weight_sum, numerator)


def attend_all(
    query_block, fresh_block, received, fetch_index, page_here, lengths, live_rows, causal, fresh_on
):
    kv_width = received.shape[-1]
    heads_kv = kv_width // HD
    row_count = query_block.shape[1]
    group_size = query_block.shape[2] // kv_width
    page_count = fetch_index.shape[1]
    positions = jnp.arange(page_count * PAGE, dtype=jnp.int32)

    def one_sequence(inputs):
        query_rows, fresh_rows, index_row, here_row, length, live_row = inputs
        fetched = jnp.take(received, index_row, axis=0)
        cache_keys = fetched[:, 0].reshape(page_count * PAGE, heads_kv, HD)
        cache_values = fetched[:, 1].reshape(page_count * PAGE, heads_kv, HD)
        page_mask = jnp.broadcast_to(here_row[:, None], (page_count, PAGE)).reshape(
            page_count * PAGE
        )
        cache_valid = page_mask & (positions < length)
        query_heads = query_rows.reshape(row_count, heads_kv, group_size, HD)
        fresh_keys = fresh_rows[:, 0].reshape(row_count, heads_kv, HD)
        fresh_values = fresh_rows[:, 1].reshape(row_count, heads_kv, HD)
        fresh_valid = causal & live_row[:, None] & fresh_on
        return partial_softmax(
            query_heads,
            cache_keys,
            cache_values,
            cache_valid,
            fresh_keys,
            fresh_values,
            fresh_valid,
        )

    return lax.map(
        one_sequence, (query_block, fresh_block, fetch_index, page_here, lengths, live_rows)
    )


def finish(weight_sum, numerator, live_rows):
    unused_rows = 1.0 - live_rows.astype(jnp.float32)
    attended = numerator / (weight_sum + unused_rows[:, None, None, :])[..., None]
    attended = jnp.where(live_rows[:, None, None, :, None], attended, 0.0)
    seq_dev, heads_kv, group_size, row_count, head_dim = attended.shape
    return (
        jnp.transpose(attended, (0, 3, 1, 2, 4))
        .reshape(seq_dev, row_count, heads_kv * group_size * head_dim)
        .astype(jnp.bfloat16)
    )


def exchange_pages(queries, new_kv, kv_pages, page_table, cached_len, is_prefill):
    seq_shards = lax.axis_size("seq")
    sub_count = lax.axis_size("sub")
    owners = seq_shards * sub_count
    seq_index = lax.axis_index("seq")
    core_index = lax.axis_index("sub")
    owner_self = seq_index * sub_count + core_index
    seq_dev, row_count, query_width = queries.shape
    pages_dev = kv_pages.shape[0]
    kv_width = kv_pages.shape[3]
    page_count = page_table.shape[1]
    entries = seq_dev * page_count
    capacity = (entries + owners - 1) // owners
    table_rows = page_table.reshape(seq_shards, entries)
    holder = jnp.where(table_rows >= 0, table_rows // pages_dev, -1)
    slot_of = jnp.where(table_rows >= 0, table_rows % pages_dev, 0)
    owned_here = holder == owner_self
    rank_among = jnp.cumsum(owned_here.astype(jnp.int32), axis=1) - 1
    picked = owned_here[:, :, None] & (
        rank_among[:, :, None] == jnp.arange(capacity, dtype=jnp.int32)[None, None, :]
    )
    send_slots = jnp.sum(jnp.where(picked, slot_of[:, :, None], 0), axis=1).reshape(
        seq_shards * capacity
    )
    first_seq = seq_index * seq_dev
    my_table = lax.dynamic_slice_in_dim(page_table, first_seq, seq_dev, 0)
    my_lengths = lax.dynamic_slice_in_dim(cached_len, first_seq, seq_dev, 0)
    my_flags = lax.dynamic_slice_in_dim(is_prefill, first_seq, seq_dev, 0)
    flat_table = my_table.reshape(entries)
    my_holder = jnp.where(flat_table >= 0, flat_table // pages_dev, -1)
    entry_order = jnp.arange(entries, dtype=jnp.int32)
    earlier = (my_holder[:, None] == my_holder[None, :]) & (
        entry_order[None, :] < entry_order[:, None]
    )
    my_rank = jnp.sum(earlier.astype(jnp.int32), axis=1)
    row_ids = jnp.arange(row_count, dtype=jnp.int32)
    live_rows = (my_flags[:, None] == 1) | (row_ids[None, :] == 0)
    causal = row_ids[None, :] <= row_ids[:, None]
    part_width = kv_width // sub_count
    split_pages = kv_pages.reshape(pages_dev, 2, PAGE, sub_count, part_width)
    chosen = jnp.take(split_pages, send_slots, axis=0).reshape(
        seq_shards, capacity, 2, PAGE, sub_count, part_width
    )
    outgoing = jnp.moveaxis(chosen, 4, 1).reshape(owners, capacity, 2, PAGE, part_width)
    received = lax.all_to_all(
        outgoing, ("seq", "sub"), split_axis=0, concat_axis=0, tiled=True
    ).reshape(owners * capacity, 2, PAGE, part_width)
    present = flat_table >= 0
    fetch_index = jnp.where(present, my_holder * capacity + my_rank, 0)
    query_part = query_width // sub_count
    my_queries = lax.dynamic_slice_in_dim(queries, core_index * query_part, query_part, 2)
    my_fresh = lax.dynamic_slice_in_dim(new_kv, core_index * part_width, part_width, 3)
    peak, weight_sum, numerator = attend_all(
        my_queries,
        my_fresh,
        received,
        fetch_index.reshape(seq_dev, page_count),
        present.reshape(seq_dev, page_count),
        my_lengths,
        live_rows,
        causal,
        core_index >= 0,
    )
    own_heads = finish(weight_sum, numerator, live_rows)
    return lax.all_gather(own_heads, "sub", axis=2, tiled=True)


MESH = pl.DeviceIdType.MESH
SCALE = HD ** (-0.5)


def greet(z, n):
    has_left, has_right = z > 0, z < n - 1
    barrier = pltpu.get_barrier_semaphore()

    @pl.when(has_left)
    def _():
        pl.semaphore_signal(barrier, inc=1, device_id={"seq": z - 1}, device_id_type=MESH)

    @pl.when(has_right)
    def _():
        pl.semaphore_signal(barrier, inc=1, device_id={"seq": z + 1}, device_id_type=MESH)

    pl.semaphore_wait(barrier, has_left.astype(jnp.int32) + has_right.astype(jnp.int32))
    return has_left, has_right


def remote(src, dst, send, recv, z):
    return pltpu.make_async_remote_copy(
        src_ref=src, dst_ref=dst, send_sem=send, recv_sem=recv,
        device_id={"seq": z}, device_id_type=MESH,
    )


LAG = 2


def line_steps(z, n, count, has_left, has_right, from_left, from_right, last):
    def guarded(c, work):
        @pl.when((c >= 0) & (c < count))
        def _():
            work(c)

    def step(s, carry):
        guarded(s - LAG * z, from_left)
        guarded(s - LAG * (n - 1 - z), from_right)
        guarded(s - LAG * jnp.maximum(z, n - 1 - z), last)
        return carry

    lax.fori_loop(0, count + LAG * (n - 1), step, 0)


def gather_queries_kernel(n, count, own, out, rin, rout, lin, lout, rs, rr, ls, lr):
    z = lax.axis_index("seq")
    has_left, has_right = greet(z, n)

    def right(c):
        return remote(rout.at[c], rin.at[c], rs.at[c], rr.at[c], z + 1)

    def left(c):
        return remote(lout.at[c], lin.at[c], ls.at[c], lr.at[c], z - 1)

    def from_left(c):
        @pl.when(has_left)
        def _():
            right(c).wait_recv()
            rout[c] = own[c] + rin[c]

        @pl.when(jnp.logical_not(has_left))
        def _():
            rout[c] = own[c]

        @pl.when(has_right)
        def _():
            right(c).start()

    def from_right(c):
        @pl.when(has_right)
        def _():
            left(c).wait_recv()
            lout[c] = own[c] + lin[c]

        @pl.when(jnp.logical_not(has_right))
        def _():
            lout[c] = own[c]

        @pl.when(has_left)
        def _():
            left(c).start()

    def last(c):
        @pl.when(has_right)
        def _():
            out[c] = rout[c] + lin[c]

        @pl.when(jnp.logical_not(has_right))
        def _():
            out[c] = rout[c]

    line_steps(z, n, count, has_left, has_right, from_left, from_right, last)

    def drain(c, carry):
        @pl.when(has_right)
        def _():
            right(c).wait_send()

        @pl.when(has_left)
        def _():
            left(c).wait_send()

        return carry

    lax.fori_loop(0, count, drain, 0)


def gather_queries(own, n):
    total, width = own.shape
    rows = 48 if total % 48 == 0 else 16
    count = total // rows
    shape = (count, rows, width)
    buffer = pltpu.VMEM(shape, own.dtype)
    return pl.pallas_call(
        functools.partial(gather_queries_kernel, n, count),
        out_shape=jax.ShapeDtypeStruct(shape, own.dtype),
        in_specs=[pl.BlockSpec(memory_space=pltpu.VMEM)],
        out_specs=pl.BlockSpec(memory_space=pltpu.VMEM),
        scratch_shapes=[buffer] * 4 + [pltpu.SemaphoreType.DMA((count,))] * 4,
        compiler_params=pltpu.CompilerParams(collective_id=0, has_side_effects=True),
        name="gather_queries",
    )(own.reshape(shape)).reshape(total, width)


def merge(o1, e1, o2, e2):
    top = jnp.maximum(e1, e2)
    w1, w2 = jnp.exp(e1 - top), jnp.exp(e2 - top)
    total = w1 + w2
    inv = 1.0 / total
    return o1 * (w1 * inv) + o2 * (w2 * inv), top + jnp.log(total)


def reduce_outputs_kernel(
    n, count, o, e, out, oute, ri, ro, li, lo, rei, reo, lei, leo, rs, rr, ls, lr, res, rer, les, ler
):
    z = lax.axis_index("seq")
    has_left, has_right = greet(z, n)

    def right(c):
        return (
            remote(ro.at[c], ri.at[c], rs.at[c], rr.at[c], z + 1),
            remote(reo.at[c], rei.at[c], res.at[c], rer.at[c], z + 1),
        )

    def left(c):
        return (
            remote(lo.at[c], li.at[c], ls.at[c], lr.at[c], z - 1),
            remote(leo.at[c], lei.at[c], les.at[c], ler.at[c], z - 1),
        )

    def join(o1, e1, o2, e2, oo, eo, c):
        joined, stat = merge(o1[c].astype(jnp.float32), e1[c], o2[c].astype(jnp.float32), e2[c])
        oo[c] = joined.astype(oo.dtype)
        eo[c] = stat

    def from_left(c):
        @pl.when(has_left)
        def _():
            for x in right(c):
                x.wait_recv()
            join(o, e, ri, rei, ro, reo, c)

        @pl.when(jnp.logical_not(has_left))
        def _():
            ro[c] = o[c]
            reo[c] = e[c]

        @pl.when(has_right)
        def _():
            for x in right(c):
                x.start()

    def from_right(c):
        @pl.when(has_right)
        def _():
            for x in left(c):
                x.wait_recv()
            join(o, e, li, lei, lo, leo, c)

        @pl.when(jnp.logical_not(has_right))
        def _():
            lo[c] = o[c]
            leo[c] = e[c]

        @pl.when(has_left)
        def _():
            for x in left(c):
                x.start()

    def last(c):
        @pl.when(has_right)
        def _():
            join(ro, reo, li, lei, out, oute, c)

        @pl.when(jnp.logical_not(has_right))
        def _():
            out[c] = ro[c]
            oute[c] = reo[c]

    line_steps(z, n, count, has_left, has_right, from_left, from_right, last)

    def drain(c, carry):
        @pl.when(has_right)
        def _():
            for x in right(c):
                x.wait_send()

        @pl.when(has_left)
        def _():
            for x in left(c):
                x.wait_send()

        return carry

    lax.fori_loop(0, count, drain, 0)


def reduce_outputs(o, e, n):
    count = e.shape[0]
    return pl.pallas_call(
        functools.partial(reduce_outputs_kernel, n, count),
        out_shape=[jax.ShapeDtypeStruct(x.shape, x.dtype) for x in (o, e)],
        in_specs=[pl.BlockSpec(memory_space=pltpu.VMEM)] * 2,
        out_specs=[pl.BlockSpec(memory_space=pltpu.VMEM)] * 2,
        scratch_shapes=[pltpu.VMEM(o.shape, o.dtype)] * 4
        + [pltpu.VMEM(e.shape, e.dtype)] * 4
        + [pltpu.SemaphoreType.DMA((count,))] * 8,
        compiler_params=pltpu.CompilerParams(collective_id=1, has_side_effects=True),
        name="reduce_outputs",
    )(o, e)[0]


def stacked_heads(rows, k, group_size):
    return jnp.concatenate(
        [rows[:, (k * group_size + g) * HD : (k * group_size + g + 1) * HD] for g in range(group_size)], axis=0
    )


def scores_of(keys, query):
    return (
        lax.dot_general(keys, query, (((1,), (1,)), ((), ())), preferred_element_type=jnp.float32) * SCALE
    )


def partial_outputs(query, blocks):
    scored = [jnp.where(mask, scores_of(keys, query), NEG_FILL) for keys, _, mask in blocks]
    peak = functools.reduce(jnp.maximum, [jnp.max(s, axis=0, keepdims=True) for s in scored])
    acc, total = None, None
    for s, (_, values, mask) in zip(scored, blocks):
        weights = jnp.where(mask, jnp.exp(s - peak), 0.0)
        part = jnp.sum(weights, axis=0, keepdims=True)
        prod = lax.dot_general(
            values, weights.astype(jnp.bfloat16), (((0,), (0,)), ((), ())), preferred_element_type=jnp.float32
        )
        acc = prod if acc is None else acc + prod
        total = part if total is None else total + part
    empty = total == 0.0
    total = jnp.where(empty, 1.0, total)
    return acc * (1.0 / total), jnp.where(empty, NEG_FILL, peak + jnp.log(total))


def prefill_kernel(most, heads, group_size, pages, valid, home, local, q_ref, *refs):
    page_refs, (fk_ref, fv_ref, o_ref, e_ref) = refs[:most], refs[most:]
    j = pl.program_id(0)
    rows = q_ref.shape[0]
    lanes = group_size * rows
    key_id = lax.broadcasted_iota(jnp.int32, (PAGE, 1), 0)
    fresh_id = lax.broadcasted_iota(jnp.int32, (rows, lanes), 0)
    lane_row = lax.broadcasted_iota(jnp.int32, (rows, lanes), 1) % rows
    for k in range(heads):
        cols = slice(k * HD, (k + 1) * HD)
        query = stacked_heads(q_ref, k, group_size)
        blocks = [
            (ref[0, 0, :, cols], ref[0, 1, :, cols], key_id < valid[j, i]) for i, ref in enumerate(page_refs)
        ]
        fresh_mask = (fresh_id <= lane_row) & (home[j] == 1)
        blocks.append((fk_ref[0, :, cols], fv_ref[0, :, cols], fresh_mask))
        o, e = partial_outputs(query, blocks)
        o_ref[k] = o.astype(o_ref.dtype)
        e_ref[k] = e


def decode_kernel(most, heads, group_size, seqs, pages, valid, home, local, seq, q_ref, *refs):
    page_refs, (fk_ref, fv_ref, _, _, o_ref, e_ref) = refs[:most], refs[most:]
    j = pl.program_id(0)
    lanes = group_size * seqs
    fresh_rows = 16
    key_id = lax.broadcasted_iota(jnp.int32, (PAGE, 1), 0)
    fresh_id = lax.broadcasted_iota(jnp.int32, (fresh_rows, 1), 0)
    mine = lax.broadcasted_iota(jnp.int32, (1, lanes), 1) % seqs == seq[j]

    @pl.when(j == 0)
    def _():
        o_ref[...] = jnp.zeros_like(o_ref)
        e_ref[...] = jnp.full_like(e_ref, NEG_FILL)

    for k in range(heads):
        cols = slice(k * HD, (k + 1) * HD)
        query = stacked_heads(q_ref, k, group_size)
        blocks = [
            (ref[0, 0, :, cols], ref[0, 1, :, cols], key_id < valid[j, i]) for i, ref in enumerate(page_refs)
        ]
        fresh_mask = fresh_id < home[j]
        blocks.append((fk_ref[0, :fresh_rows, cols], fv_ref[0, :fresh_rows, cols], fresh_mask))
        o, e = partial_outputs(query, blocks)
        place = slice(k * lanes, (k + 1) * lanes)
        o_ref[0, :, place] = jnp.where(mine, o, o_ref[0, :, place].astype(jnp.float32)).astype(o_ref.dtype)
        e_ref[0, :, place] = jnp.where(mine, e, e_ref[0, :, place])


def finish_kernel(heads, group_size, seqs, slot, flag, first, o_ref, od_ref, out_ref):
    i = pl.program_id(0)
    rows = out_ref.shape[1]

    @pl.when(flag[i] == 1)
    def _():
        for k in range(heads):
            turned = o_ref[k].astype(jnp.float32).T.astype(out_ref.dtype)
            for g in range(group_size):
                h = k * group_size + g
                out_ref[0, :, h * HD : (h + 1) * HD] = turned[g * rows : (g + 1) * rows]

    @pl.when(flag[i] != 1)
    def _():
        top = lax.broadcasted_iota(jnp.int32, (rows, 1), 0) == 0
        pick = lax.broadcasted_iota(jnp.int32, (seqs, 1), 0) == first[0] + i
        for k in range(heads):
            place = slice(k * seqs * group_size, (k + 1) * seqs * group_size)
            turned = od_ref[0, :, place].astype(jnp.float32).T
            for g in range(group_size):
                h = k * group_size + g
                line = jnp.sum(jnp.where(pick, turned[g * seqs : (g + 1) * seqs], 0.0), axis=0, keepdims=True)
                out_ref[0, :, h * HD : (h + 1) * HD] = jnp.where(top, line, 0.0).astype(out_ref.dtype)


def move_queries(queries, new_kv, kv_pages, page_table, cached_len, is_prefill):
    n = lax.axis_size("seq")
    sub_count = lax.axis_size("sub")
    z = lax.axis_index("seq")
    core = lax.axis_index("sub")
    seq_dev, row_count, query_width = queries.shape
    pages_dev, kv_width = kv_pages.shape[0], kv_pages.shape[3]
    seqs, page_count = page_table.shape
    owners = n * sub_count
    most = sub_count * (page_count // owners)
    slots = seqs // 2
    group_size = query_width // kv_width
    part_width, query_part = kv_width // sub_count, query_width // sub_count
    heads = part_width // HD

    other = (core + 1) % sub_count
    away = lax.dynamic_slice_in_dim(kv_pages, other * part_width, part_width, 3)
    here = lax.dynamic_slice_in_dim(kv_pages, core * part_width, part_width, 3)
    came = lax.ppermute(away, "sub", [(c, (c + 1) % sub_count) for c in range(sub_count)])
    pool = jnp.concatenate([here, came], axis=0)

    seq_ids = jnp.arange(seqs, dtype=jnp.int32)
    owner = page_table // pages_dev
    mine = (page_table >= 0) & (owner // sub_count == z)
    index = page_table % pages_dev + jnp.where(owner % sub_count == core, 0, pages_dev)
    rank = jnp.cumsum(mine.astype(jnp.int32), axis=1) - 1
    picked = mine[:, :, None] & (rank[:, :, None] == jnp.arange(most, dtype=jnp.int32))
    tokens = jnp.clip(cached_len[:, None] - PAGE * jnp.arange(page_count, dtype=jnp.int32), 0, PAGE)
    page_rows = jnp.sum(jnp.where(picked, index[:, :, None], 0), axis=1)
    valid_rows = jnp.sum(jnp.where(picked, tokens[:, :, None], 0), axis=1)
    flags = is_prefill == 1
    slot_of = jnp.cumsum(flags.astype(jnp.int32)) - 1
    place_of = jnp.cumsum((~flags).astype(jnp.int32)) - 1
    slot_ids = jnp.arange(slots, dtype=jnp.int32)
    slot_seq = jnp.sum(jnp.where(flags & (slot_of == slot_ids[:, None]), seq_ids, 0), axis=1)
    rest_ids = jnp.arange(seqs - slots, dtype=jnp.int32)
    rest_seq = jnp.sum(jnp.where(~flags & (place_of == rest_ids[:, None]), seq_ids, 0), axis=1)

    def tables(which):
        at_home = (which // seq_dev == z).astype(jnp.int32)
        return page_rows[which], valid_rows[which], at_home, jnp.where(at_home == 1, which % seq_dev, 0)

    slot_tables, rest_tables = tables(slot_seq), tables(rest_seq)
    my_queries = lax.dynamic_slice_in_dim(queries, core * query_part, query_part, 2)
    own_slots = jnp.where((slot_tables[2] == 1)[:, None, None], my_queries[slot_tables[3]], 0)
    first_rows = jnp.where(
        (seq_ids // seq_dev == z)[:, None], jnp.tile(my_queries[:, 0], (n, 1)), 0
    )
    own = jnp.concatenate([own_slots.reshape(slots * row_count, query_part), first_rows], axis=0)
    gathered = gather_queries(own.astype(queries.dtype), n)

    my_fresh = lax.dynamic_slice_in_dim(new_kv, core * part_width, part_width, 3)
    fresh_keys, fresh_values = my_fresh[:, :, 0], my_fresh[:, :, 1]
    lanes = group_size * row_count
    count = slots * heads + 1

    def page_spec(i):
        return pl.BlockSpec((1, 2, PAGE, part_width), lambda j, pages, *_: (pages[j, i], 0, 0, 0))

    fresh_spec = pl.BlockSpec(
        (1, row_count, part_width), lambda j, pages, valid, home, local, *_: (local[j], 0, 0)
    )
    o, e = pl.pallas_call(
        functools.partial(prefill_kernel, most, heads, group_size),
        grid_spec=pltpu.PrefetchScalarGridSpec(
            num_scalar_prefetch=4,
            grid=(slots,),
            in_specs=[pl.BlockSpec((row_count, query_part), lambda j, *_: (j, 0))]
            + [page_spec(i) for i in range(most)]
            + [fresh_spec] * 2,
            out_specs=[
                pl.BlockSpec((heads, HD, lanes), lambda j, *_: (j, 0, 0)),
                pl.BlockSpec((heads, 1, lanes), lambda j, *_: (j, 0, 0)),
            ],
        ),
        out_shape=[
            jax.ShapeDtypeStruct((count, HD, lanes), jnp.bfloat16),
            jax.ShapeDtypeStruct((count, 1, lanes), jnp.float32),
        ],
        name="prefill_attention",
    )(*slot_tables, gathered, *([pool] * most), fresh_keys, fresh_values)
    o, e = pl.pallas_call(
        functools.partial(decode_kernel, most, heads, group_size, seqs),
        grid_spec=pltpu.PrefetchScalarGridSpec(
            num_scalar_prefetch=5,
            grid=(seqs - slots,),
            in_specs=[pl.BlockSpec((seqs, query_part), lambda j, *_: (slots * row_count // seqs, 0))]
            + [page_spec(i) for i in range(most)]
            + [fresh_spec] * 2
            + [pl.BlockSpec(memory_space=pl.ANY)] * 2,
            out_specs=[
                pl.BlockSpec((1, HD, lanes), lambda j, *_: (count - 1, 0, 0)),
                pl.BlockSpec((1, 1, lanes), lambda j, *_: (count - 1, 0, 0)),
            ],
        ),
        out_shape=[jax.ShapeDtypeStruct(x.shape, x.dtype) for x in (o, e)],
        input_output_aliases={8 + most: 0, 9 + most: 1},
        name="decode_attention",
    )(*rest_tables, rest_seq, gathered, *([pool] * most), fresh_keys, fresh_values, o, e)
    o = reduce_outputs(o, e, n)

    first_seq = z * seq_dev
    my_flags = lax.dynamic_slice_in_dim(is_prefill, first_seq, seq_dev, 0)
    my_slots = jnp.maximum(lax.dynamic_slice_in_dim(slot_of, first_seq, seq_dev, 0), 0)
    own_heads = pl.pallas_call(
        functools.partial(finish_kernel, heads, group_size, seqs),
        grid_spec=pltpu.PrefetchScalarGridSpec(
            num_scalar_prefetch=3,
            grid=(seq_dev,),
            in_specs=[
                pl.BlockSpec((heads, HD, lanes), lambda i, slot, *_: (slot[i], 0, 0)),
                pl.BlockSpec((1, HD, lanes), lambda i, *_: (count - 1, 0, 0)),
            ],
            out_specs=pl.BlockSpec((1, row_count, query_part), lambda i, *_: (i, 0, 0)),
        ),
        out_shape=jax.ShapeDtypeStruct((seq_dev, row_count, query_part), jnp.bfloat16),
        name="finish",
    )(my_slots, my_flags, jnp.reshape(first_seq, (1,)).astype(jnp.int32), o, o)
    return lax.all_gather(own_heads, "sub", axis=2, tiled=True)


def per_device(queries, new_kv, kv_pages, page_table, cached_len, is_prefill):
    owners = lax.axis_size("seq") * lax.axis_size("sub")
    if page_table.shape[1] >= owners:
        return move_queries(queries, new_kv, kv_pages, page_table, cached_len, is_prefill)
    return exchange_pages(queries, new_kv, kv_pages, page_table, cached_len, is_prefill)


def solution(mesh):
    placed = (
        P(("groups", "seq"), None, "head"),
        P(("groups", "seq"), None, None, "head"),
        P(("groups", "seq", "sub"), None, None, "head"),
        P("groups", None),
        P("groups"),
        P("groups"),
    )
    return jax.shard_map(
        per_device,
        mesh=mesh,
        in_specs=placed,
        out_specs=P(("groups", "seq"), None, "head"),
        check_vma=False,
    )
```

```python
import functools

import jax
import jax.numpy as jnp
from jax import lax
from jax.experimental import pallas as pl
from jax.experimental.pallas import tpu as pltpu
from jax.sharding import PartitionSpec as P

HD = 128
PAGE = 128


NEG_FILL = -1e30


def partial_softmax(
    query_heads, cache_keys, cache_values, cache_valid, fresh_keys, fresh_values, fresh_valid
):
    score_scale = HD ** (-0.5)
    cache_scores = (
        jnp.einsum("rkgd,nkd->kgrn", query_heads, cache_keys, preferred_element_type=jnp.float32)
        * score_scale
    )
    fresh_scores = (
        jnp.einsum("rkgd,jkd->kgrj", query_heads, fresh_keys, preferred_element_type=jnp.float32)
        * score_scale
    )
    cache_mask = cache_valid[None, None, None, :]
    fresh_mask = fresh_valid[None, None, :, :]
    peak = jnp.maximum(
        jnp.max(jnp.where(cache_mask, cache_scores, NEG_FILL), axis=-1),
        jnp.max(jnp.where(fresh_mask, fresh_scores, NEG_FILL), axis=-1),
    )
    cache_weights = jnp.where(cache_mask, jnp.exp(cache_scores - peak[..., None]), 0.0)
    fresh_weights = jnp.where(fresh_mask, jnp.exp(fresh_scores - peak[..., None]), 0.0)
    weight_sum = jnp.sum(cache_weights, axis=-1) + jnp.sum(fresh_weights, axis=-1)
    numerator = jnp.einsum(
        "kgrn,nkd->kgrd",
        cache_weights.astype(jnp.bfloat16),
        cache_values,
        preferred_element_type=jnp.float32,
    )
    numerator = numerator + jnp.einsum(
        "kgrj,jkd->kgrd",
        fresh_weights.astype(jnp.bfloat16),
        fresh_values,
        preferred_element_type=jnp.float32,
    )
    return (peak, weight_sum, numerator)


def attend_all(
    query_block, fresh_block, received, fetch_index, page_here, lengths, live_rows, causal, fresh_on
):
    kv_width = received.shape[-1]
    heads_kv = kv_width // HD
    row_count = query_block.shape[1]
    group_size = query_block.shape[2] // kv_width
    page_count = fetch_index.shape[1]
    positions = jnp.arange(page_count * PAGE, dtype=jnp.int32)

    def one_sequence(inputs):
        query_rows, fresh_rows, index_row, here_row, length, live_row = inputs
        fetched = jnp.take(received, index_row, axis=0)
        cache_keys = fetched[:, 0].reshape(page_count * PAGE, heads_kv, HD)
        cache_values = fetched[:, 1].reshape(page_count * PAGE, heads_kv, HD)
        page_mask = jnp.broadcast_to(here_row[:, None], (page_count, PAGE)).reshape(
            page_count * PAGE
        )
        cache_valid = page_mask & (positions < length)
        query_heads = query_rows.reshape(row_count, heads_kv, group_size, HD)
        fresh_keys = fresh_rows[:, 0].reshape(row_count, heads_kv, HD)
        fresh_values = fresh_rows[:, 1].reshape(row_count, heads_kv, HD)
        fresh_valid = causal & live_row[:, None] & fresh_on
        return partial_softmax(
            query_heads,
            cache_keys,
            cache_values,
            cache_valid,
            fresh_keys,
            fresh_values,
            fresh_valid,
        )

    return lax.map(
        one_sequence, (query_block, fresh_block, fetch_index, page_here, lengths, live_rows)
    )


def finish(weight_sum, numerator, live_rows):
    unused_rows = 1.0 - live_rows.astype(jnp.float32)
    attended = numerator / (weight_sum + unused_rows[:, None, None, :])[..., None]
    attended = jnp.where(live_rows[:, None, None, :, None], attended, 0.0)
    seq_dev, heads_kv, group_size, row_count, head_dim = attended.shape
    return (
        jnp.transpose(attended, (0, 3, 1, 2, 4))
        .reshape(seq_dev, row_count, heads_kv * group_size * head_dim)
        .astype(jnp.bfloat16)
    )


def exchange_pages(queries, new_kv, kv_pages, page_table, cached_len, is_prefill):
    seq_shards = lax.axis_size("seq")
    sub_count = lax.axis_size("sub")
    owners = seq_shards * sub_count
    seq_index = lax.axis_index("seq")
    core_index = lax.axis_index("sub")
    owner_self = seq_index * sub_count + core_index
    seq_dev, row_count, query_width = queries.shape
    pages_dev = kv_pages.shape[0]
    kv_width = kv_pages.shape[3]
    page_count = page_table.shape[1]
    entries = seq_dev * page_count
    capacity = (entries + owners - 1) // owners
    table_rows = page_table.reshape(seq_shards, entries)
    holder = jnp.where(table_rows >= 0, table_rows // pages_dev, -1)
    slot_of = jnp.where(table_rows >= 0, table_rows % pages_dev, 0)
    owned_here = holder == owner_self
    rank_among = jnp.cumsum(owned_here.astype(jnp.int32), axis=1) - 1
    picked = owned_here[:, :, None] & (
        rank_among[:, :, None] == jnp.arange(capacity, dtype=jnp.int32)[None, None, :]
    )
    send_slots = jnp.sum(jnp.where(picked, slot_of[:, :, None], 0), axis=1).reshape(
        seq_shards * capacity
    )
    first_seq = seq_index * seq_dev
    my_table = lax.dynamic_slice_in_dim(page_table, first_seq, seq_dev, 0)
    my_lengths = lax.dynamic_slice_in_dim(cached_len, first_seq, seq_dev, 0)
    my_flags = lax.dynamic_slice_in_dim(is_prefill, first_seq, seq_dev, 0)
    flat_table = my_table.reshape(entries)
    my_holder = jnp.where(flat_table >= 0, flat_table // pages_dev, -1)
    entry_order = jnp.arange(entries, dtype=jnp.int32)
    earlier = (my_holder[:, None] == my_holder[None, :]) & (
        entry_order[None, :] < entry_order[:, None]
    )
    my_rank = jnp.sum(earlier.astype(jnp.int32), axis=1)
    row_ids = jnp.arange(row_count, dtype=jnp.int32)
    live_rows = (my_flags[:, None] == 1) | (row_ids[None, :] == 0)
    causal = row_ids[None, :] <= row_ids[:, None]
    part_width = kv_width // sub_count
    split_pages = kv_pages.reshape(pages_dev, 2, PAGE, sub_count, part_width)
    chosen = jnp.take(split_pages, send_slots, axis=0).reshape(
        seq_shards, capacity, 2, PAGE, sub_count, part_width
    )
    outgoing = jnp.moveaxis(chosen, 4, 1).reshape(owners, capacity, 2, PAGE, part_width)
    received = lax.all_to_all(
        outgoing, ("seq", "sub"), split_axis=0, concat_axis=0, tiled=True
    ).reshape(owners * capacity, 2, PAGE, part_width)
    present = flat_table >= 0
    fetch_index = jnp.where(present, my_holder * capacity + my_rank, 0)
    query_part = query_width // sub_count
    my_queries = lax.dynamic_slice_in_dim(queries, core_index * query_part, query_part, 2)
    my_fresh = lax.dynamic_slice_in_dim(new_kv, core_index * part_width, part_width, 3)
    peak, weight_sum, numerator = attend_all(
        my_queries,
        my_fresh,
        received,
        fetch_index.reshape(seq_dev, page_count),
        present.reshape(seq_dev, page_count),
        my_lengths,
        live_rows,
        causal,
        core_index >= 0,
    )
    own_heads = finish(weight_sum, numerator, live_rows)
    return lax.all_gather(own_heads, "sub", axis=2, tiled=True)


MESH = pl.DeviceIdType.MESH
SCALE = HD ** (-0.5)


def greet(z, n):
    has_left, has_right = z > 0, z < n - 1
    barrier = pltpu.get_barrier_semaphore()

    @pl.when(has_left)
    def _():
        pl.semaphore_signal(barrier, inc=1, device_id={"seq": z - 1}, device_id_type=MESH)

    @pl.when(has_right)
    def _():
        pl.semaphore_signal(barrier, inc=1, device_id={"seq": z + 1}, device_id_type=MESH)

    pl.semaphore_wait(barrier, has_left.astype(jnp.int32) + has_right.astype(jnp.int32))
    return has_left, has_right


def remote(src, dst, send, recv, z):
    return pltpu.make_async_remote_copy(
        src_ref=src, dst_ref=dst, send_sem=send, recv_sem=recv,
        device_id={"seq": z}, device_id_type=MESH,
    )


LAG = 2


def line_steps(z, n, count, has_left, has_right, from_left, from_right, last):
    def guarded(c, work):
        @pl.when((c >= 0) & (c < count))
        def _():
            work(c)

    def step(s, carry):
        guarded(s - LAG * z, from_left)
        guarded(s - LAG * (n - 1 - z), from_right)
        guarded(s - LAG * jnp.maximum(z, n - 1 - z), last)
        return carry

    lax.fori_loop(0, count + LAG * (n - 1), step, 0)


def gather_queries_kernel(n, count, own, out, rin, rout, lin, lout, rs, rr, ls, lr):
    z = lax.axis_index("seq")
    has_left, has_right = greet(z, n)

    def right(c):
        return remote(rout.at[c], rin.at[c], rs.at[c], rr.at[c], z + 1)

    def left(c):
        return remote(lout.at[c], lin.at[c], ls.at[c], lr.at[c], z - 1)

    def from_left(c):
        @pl.when(has_left)
        def _():
            right(c).wait_recv()
            rout[c] = own[c] + rin[c]

        @pl.when(jnp.logical_not(has_left))
        def _():
            rout[c] = own[c]

        @pl.when(has_right)
        def _():
            right(c).start()

    def from_right(c):
        @pl.when(has_right)
        def _():
            left(c).wait_recv()
            lout[c] = own[c] + lin[c]

        @pl.when(jnp.logical_not(has_right))
        def _():
            lout[c] = own[c]

        @pl.when(has_left)
        def _():
            left(c).start()

    def last(c):
        @pl.when(has_right)
        def _():
            out[c] = rout[c] + lin[c]

        @pl.when(jnp.logical_not(has_right))
        def _():
            out[c] = rout[c]

    line_steps(z, n, count, has_left, has_right, from_left, from_right, last)

    def drain(c, carry):
        @pl.when(has_right)
        def _():
            right(c).wait_send()

        @pl.when(has_left)
        def _():
            left(c).wait_send()

        return carry

    lax.fori_loop(0, count, drain, 0)


def gather_queries(own, n):
    total, width = own.shape
    rows = 48 if total % 48 == 0 else 16
    count = total // rows
    shape = (count, rows, width)
    buffer = pltpu.VMEM(shape, own.dtype)
    return pl.pallas_call(
        functools.partial(gather_queries_kernel, n, count),
        out_shape=jax.ShapeDtypeStruct(shape, own.dtype),
        in_specs=[pl.BlockSpec(memory_space=pltpu.VMEM)],
        out_specs=pl.BlockSpec(memory_space=pltpu.VMEM),
        scratch_shapes=[buffer] * 4 + [pltpu.SemaphoreType.DMA((count,))] * 4,
        compiler_params=pltpu.CompilerParams(collective_id=0, has_side_effects=True),
        name="gather_queries",
    )(own.reshape(shape)).reshape(total, width)


def merge(o1, e1, o2, e2):
    top = jnp.maximum(e1, e2)
    w1, w2 = jnp.exp(e1 - top), jnp.exp(e2 - top)
    total = w1 + w2
    inv = 1.0 / total
    return o1 * (w1 * inv) + o2 * (w2 * inv), top + jnp.log(total)


def reduce_outputs_kernel(
    n, count, o, e, out, oute, ri, ro, li, lo, rei, reo, lei, leo, rs, rr, ls, lr, res, rer, les, ler
):
    z = lax.axis_index("seq")
    has_left, has_right = greet(z, n)

    def right(c):
        return (
            remote(ro.at[c], ri.at[c], rs.at[c], rr.at[c], z + 1),
            remote(reo.at[c], rei.at[c], res.at[c], rer.at[c], z + 1),
        )

    def left(c):
        return (
            remote(lo.at[c], li.at[c], ls.at[c], lr.at[c], z - 1),
            remote(leo.at[c], lei.at[c], les.at[c], ler.at[c], z - 1),
        )

    def join(o1, e1, o2, e2, oo, eo, c):
        joined, stat = merge(o1[c].astype(jnp.float32), e1[c], o2[c].astype(jnp.float32), e2[c])
        oo[c] = joined.astype(oo.dtype)
        eo[c] = stat

    def from_left(c):
        @pl.when(has_left)
        def _():
            for x in right(c):
                x.wait_recv()
            join(o, e, ri, rei, ro, reo, c)

        @pl.when(jnp.logical_not(has_left))
        def _():
            ro[c] = o[c]
            reo[c] = e[c]

        @pl.when(has_right)
        def _():
            for x in right(c):
                x.start()

    def from_right(c):
        @pl.when(has_right)
        def _():
            for x in left(c):
                x.wait_recv()
            join(o, e, li, lei, lo, leo, c)

        @pl.when(jnp.logical_not(has_right))
        def _():
            lo[c] = o[c]
            leo[c] = e[c]

        @pl.when(has_left)
        def _():
            for x in left(c):
                x.start()

    def last(c):
        @pl.when(has_right)
        def _():
            join(ro, reo, li, lei, out, oute, c)

        @pl.when(jnp.logical_not(has_right))
        def _():
            out[c] = ro[c]
            oute[c] = reo[c]

    line_steps(z, n, count, has_left, has_right, from_left, from_right, last)

    def drain(c, carry):
        @pl.when(has_right)
        def _():
            for x in right(c):
                x.wait_send()

        @pl.when(has_left)
        def _():
            for x in left(c):
                x.wait_send()

        return carry

    lax.fori_loop(0, count, drain, 0)


def reduce_outputs(o, e, n):
    count = e.shape[0]
    return pl.pallas_call(
        functools.partial(reduce_outputs_kernel, n, count),
        out_shape=[jax.ShapeDtypeStruct(x.shape, x.dtype) for x in (o, e)],
        in_specs=[pl.BlockSpec(memory_space=pltpu.VMEM)] * 2,
        out_specs=[pl.BlockSpec(memory_space=pltpu.VMEM)] * 2,
        scratch_shapes=[pltpu.VMEM(o.shape, o.dtype)] * 4
        + [pltpu.VMEM(e.shape, e.dtype)] * 4
        + [pltpu.SemaphoreType.DMA((count,))] * 8,
        compiler_params=pltpu.CompilerParams(collective_id=1, has_side_effects=True),
        name="reduce_outputs",
    )(o, e)[0]


def stacked_heads(rows, k, group_size):
    return jnp.concatenate(
        [rows[:, (k * group_size + g) * HD : (k * group_size + g + 1) * HD] for g in range(group_size)], axis=0
    )


def scores_of(keys, query):
    return (
        lax.dot_general(keys, query, (((1,), (1,)), ((), ())), preferred_element_type=jnp.float32) * SCALE
    )


def partial_outputs(query, blocks):
    scored = [jnp.where(mask, scores_of(keys, query), NEG_FILL) for keys, _, mask in blocks]
    peak = functools.reduce(jnp.maximum, [jnp.max(s, axis=0, keepdims=True) for s in scored])
    peak = jnp.maximum(peak, 0.1 * NEG_FILL)
    acc, total = None, None
    for s, (_, values, _) in zip(scored, blocks):
        weights = jnp.exp(s - peak)
        part = jnp.sum(weights, axis=0, keepdims=True)
        prod = lax.dot_general(
            values, weights.astype(jnp.bfloat16), (((0,), (0,)), ((), ())), preferred_element_type=jnp.float32
        )
        acc = prod if acc is None else acc + prod
        total = part if total is None else total + part
    empty = total == 0.0
    total = jnp.where(empty, 1.0, total)
    return acc * (1.0 / total), jnp.where(empty, NEG_FILL, peak + jnp.log(total))


def prefill_kernel(most, heads, group_size, pages, valid, home, local, q_ref, *refs):
    page_refs, (fk_ref, fv_ref, o_ref, e_ref) = refs[:most], refs[most:]
    j = pl.program_id(0)
    rows = q_ref.shape[0]
    lanes = group_size * rows
    key_id = lax.broadcasted_iota(jnp.int32, (PAGE, 1), 0)
    fresh_id = lax.broadcasted_iota(jnp.int32, (rows, lanes), 0)
    lane_row = lax.broadcasted_iota(jnp.int32, (rows, lanes), 1) % rows
    for k in range(heads):
        cols = slice(k * HD, (k + 1) * HD)
        query = stacked_heads(q_ref, k, group_size)
        blocks = [
            (ref[0, 0, :, cols], ref[0, 1, :, cols], key_id < valid[j, i]) for i, ref in enumerate(page_refs)
        ]
        fresh_mask = (fresh_id <= lane_row) & (home[j] == 1)
        blocks.append((fk_ref[0, :, cols], fv_ref[0, :, cols], fresh_mask))
        o, e = partial_outputs(query, blocks)
        o_ref[k] = o.astype(o_ref.dtype)
        e_ref[k] = e


def decode_kernel(most, heads, group_size, seqs, pages, valid, home, local, seq, q_ref, *refs):
    page_refs, (fk_ref, fv_ref, _, _, o_ref, e_ref) = refs[:most], refs[most:]
    j = pl.program_id(0)
    lanes = group_size * seqs
    fresh_rows = 16
    key_id = lax.broadcasted_iota(jnp.int32, (PAGE, 1), 0)
    fresh_id = lax.broadcasted_iota(jnp.int32, (fresh_rows, 1), 0)
    mine = lax.broadcasted_iota(jnp.int32, (1, lanes), 1) % seqs == seq[j]

    @pl.when(j == 0)
    def _():
        o_ref[...] = jnp.zeros_like(o_ref)
        e_ref[...] = jnp.full_like(e_ref, NEG_FILL)

    for k in range(heads):
        cols = slice(k * HD, (k + 1) * HD)
        query = stacked_heads(q_ref, k, group_size)
        blocks = [
            (ref[0, 0, :, cols], ref[0, 1, :, cols], key_id < valid[j, i]) for i, ref in enumerate(page_refs)
        ]
        fresh_mask = fresh_id < home[j]
        blocks.append((fk_ref[0, :fresh_rows, cols], fv_ref[0, :fresh_rows, cols], fresh_mask))
        o, e = partial_outputs(query, blocks)
        place = slice(k * lanes, (k + 1) * lanes)
        o_ref[0, :, place] = jnp.where(mine, o, o_ref[0, :, place].astype(jnp.float32)).astype(o_ref.dtype)
        e_ref[0, :, place] = jnp.where(mine, e, e_ref[0, :, place])


def finish_kernel(heads, group_size, seqs, slot, flag, first, o_ref, od_ref, out_ref):
    i = pl.program_id(0)
    rows = out_ref.shape[1]

    @pl.when(flag[i] == 1)
    def _():
        for k in range(heads):
            turned = o_ref[k].astype(jnp.float32).T.astype(out_ref.dtype)
            for g in range(group_size):
                h = k * group_size + g
                out_ref[0, :, h * HD : (h + 1) * HD] = turned[g * rows : (g + 1) * rows]

    @pl.when(flag[i] != 1)
    def _():
        top = lax.broadcasted_iota(jnp.int32, (rows, 1), 0) == 0
        pick = lax.broadcasted_iota(jnp.int32, (seqs, 1), 0) == first[0] + i
        for k in range(heads):
            place = slice(k * seqs * group_size, (k + 1) * seqs * group_size)
            turned = od_ref[0, :, place].astype(jnp.float32).T
            for g in range(group_size):
                h = k * group_size + g
                line = jnp.sum(jnp.where(pick, turned[g * seqs : (g + 1) * seqs], 0.0), axis=0, keepdims=True)
                out_ref[0, :, h * HD : (h + 1) * HD] = jnp.where(top, line, 0.0).astype(out_ref.dtype)


def move_queries(queries, new_kv, kv_pages, page_table, cached_len, is_prefill):
    n = lax.axis_size("seq")
    sub_count = lax.axis_size("sub")
    z = lax.axis_index("seq")
    core = lax.axis_index("sub")
    seq_dev, row_count, query_width = queries.shape
    pages_dev, kv_width = kv_pages.shape[0], kv_pages.shape[3]
    seqs, page_count = page_table.shape
    owners = n * sub_count
    each = page_count // owners
    most = sub_count * each
    slots = seqs // 2
    group_size = query_width // kv_width
    part_width, query_part = kv_width // sub_count, query_width // sub_count
    heads = part_width // HD

    other = (core + 1) % sub_count
    away = lax.dynamic_slice_in_dim(kv_pages, other * part_width, part_width, 3)
    came = lax.ppermute(away, "sub", [(c, (c + 1) % sub_count) for c in range(sub_count)])

    seq_ids = jnp.arange(seqs, dtype=jnp.int32)
    owner = jnp.where(page_table >= 0, page_table // pages_dev, -1)
    sources = z * sub_count + jnp.stack([core, other])
    mine = owner[None] == sources[:, None, None]
    rank = jnp.cumsum(mine.astype(jnp.int32), axis=2) - 1
    picked = mine[..., None] & (rank[..., None] == jnp.arange(each, dtype=jnp.int32))
    tokens = jnp.clip(cached_len[:, None] - PAGE * jnp.arange(page_count, dtype=jnp.int32), 0, PAGE)

    def listed(values):
        found = jnp.sum(jnp.where(picked, values[None, :, :, None], 0), axis=2)
        return jnp.moveaxis(found, 0, 1).reshape(seqs, most)

    page_rows, valid_rows = listed(page_table % pages_dev), listed(tokens)
    flags = is_prefill == 1
    slot_of = jnp.cumsum(flags.astype(jnp.int32)) - 1
    place_of = jnp.cumsum((~flags).astype(jnp.int32)) - 1
    slot_ids = jnp.arange(slots, dtype=jnp.int32)
    slot_seq = jnp.sum(jnp.where(flags & (slot_of == slot_ids[:, None]), seq_ids, 0), axis=1)
    rest_ids = jnp.arange(seqs - slots, dtype=jnp.int32)
    rest_seq = jnp.sum(jnp.where(~flags & (place_of == rest_ids[:, None]), seq_ids, 0), axis=1)

    def tables(which):
        at_home = (which // seq_dev == z).astype(jnp.int32)
        places = jnp.where(at_home == 1, which % seq_dev, 0)
        chosen = which[:, None, None] == seq_ids[None, :, None]
        rows = [jnp.sum(jnp.where(chosen, x[None], 0), axis=1) for x in (page_rows, valid_rows)]
        return rows[0], rows[1], at_home, jnp.append(places, core)

    slot_tables, rest_tables = tables(slot_seq), tables(rest_seq)
    my_queries = lax.dynamic_slice_in_dim(queries, core * query_part, query_part, 2)
    own_slots = jnp.where((slot_tables[2] == 1)[:, None, None], my_queries[slot_tables[3][:slots]], 0)
    first_rows = jnp.where(
        (seq_ids // seq_dev == z)[:, None], jnp.tile(my_queries[:, 0], (n, 1)), 0
    )
    own = jnp.concatenate([own_slots.reshape(slots * row_count, query_part), first_rows], axis=0)
    gathered = gather_queries(own.astype(queries.dtype), n)

    my_fresh = lax.dynamic_slice_in_dim(new_kv, core * part_width, part_width, 3)
    fresh_keys, fresh_values = my_fresh[:, :, 0], my_fresh[:, :, 1]
    lanes = group_size * row_count
    count = slots * heads + 1

    def page_spec(i):
        if i >= each:
            return pl.BlockSpec((1, 2, PAGE, part_width), lambda j, pages, *_: (pages[j, i], 0, 0, 0))
        return pl.BlockSpec(
            (1, 2, PAGE, part_width),
            lambda j, pages, valid, home, local, *_: (pages[j, i], 0, 0, local[local.shape[0] - 1]),
        )

    fresh_spec = pl.BlockSpec(
        (1, row_count, part_width), lambda j, pages, valid, home, local, *_: (local[j], 0, 0)
    )
    o, e = pl.pallas_call(
        functools.partial(prefill_kernel, most, heads, group_size),
        grid_spec=pltpu.PrefetchScalarGridSpec(
            num_scalar_prefetch=4,
            grid=(slots,),
            in_specs=[pl.BlockSpec((row_count, query_part), lambda j, *_: (j, 0))]
            + [page_spec(i) for i in range(most)]
            + [fresh_spec] * 2,
            out_specs=[
                pl.BlockSpec((heads, HD, lanes), lambda j, *_: (j, 0, 0)),
                pl.BlockSpec((heads, 1, lanes), lambda j, *_: (j, 0, 0)),
            ],
        ),
        out_shape=[
            jax.ShapeDtypeStruct((count, HD, lanes), jnp.bfloat16),
            jax.ShapeDtypeStruct((count, 1, lanes), jnp.float32),
        ],
        name="prefill_attention",
    )(*slot_tables, gathered, *([kv_pages] * each), *([came] * (most - each)), fresh_keys, fresh_values)
    o, e = pl.pallas_call(
        functools.partial(decode_kernel, most, heads, group_size, seqs),
        grid_spec=pltpu.PrefetchScalarGridSpec(
            num_scalar_prefetch=5,
            grid=(seqs - slots,),
            in_specs=[pl.BlockSpec((seqs, query_part), lambda j, *_: (slots * row_count // seqs, 0))]
            + [page_spec(i) for i in range(most)]
            + [fresh_spec] * 2
            + [pl.BlockSpec(memory_space=pl.ANY)] * 2,
            out_specs=[
                pl.BlockSpec((1, HD, lanes), lambda j, *_: (count - 1, 0, 0)),
                pl.BlockSpec((1, 1, lanes), lambda j, *_: (count - 1, 0, 0)),
            ],
        ),
        out_shape=[jax.ShapeDtypeStruct(x.shape, x.dtype) for x in (o, e)],
        input_output_aliases={8 + most: 0, 9 + most: 1},
        name="decode_attention",
    )(*rest_tables, rest_seq, gathered, *([kv_pages] * each), *([came] * (most - each)), fresh_keys, fresh_values, o, e)
    o = reduce_outputs(o, e, n)

    first_seq = z * seq_dev
    my_flags = lax.dynamic_slice_in_dim(is_prefill, first_seq, seq_dev, 0)
    my_slots = jnp.maximum(lax.dynamic_slice_in_dim(slot_of, first_seq, seq_dev, 0), 0)
    own_heads = pl.pallas_call(
        functools.partial(finish_kernel, heads, group_size, seqs),
        grid_spec=pltpu.PrefetchScalarGridSpec(
            num_scalar_prefetch=3,
            grid=(seq_dev,),
            in_specs=[
                pl.BlockSpec((heads, HD, lanes), lambda i, slot, *_: (slot[i], 0, 0)),
                pl.BlockSpec((1, HD, lanes), lambda i, *_: (count - 1, 0, 0)),
            ],
            out_specs=pl.BlockSpec((1, row_count, query_part), lambda i, *_: (i, 0, 0)),
        ),
        out_shape=jax.ShapeDtypeStruct((seq_dev, row_count, query_part), jnp.bfloat16),
        name="finish",
    )(my_slots, my_flags, jnp.reshape(first_seq, (1,)).astype(jnp.int32), o, o)
    pairs = [(c, (c + 1) % sub_count) for c in range(sub_count)]
    came_heads = lax.ppermute(own_heads, "sub", pairs)
    first_half = jnp.where(core == 0, own_heads, came_heads)
    second_half = jnp.where(core == 0, came_heads, own_heads)
    return jnp.concatenate([first_half, second_half], axis=2)


def per_device(queries, new_kv, kv_pages, page_table, cached_len, is_prefill):
    owners = lax.axis_size("seq") * lax.axis_size("sub")
    if page_table.shape[1] >= owners:
        return move_queries(queries, new_kv, kv_pages, page_table, cached_len, is_prefill)
    return exchange_pages(queries, new_kv, kv_pages, page_table, cached_len, is_prefill)


def solution(mesh):
    placed = (
        P(("groups", "seq"), None, "head"),
        P(("groups", "seq"), None, None, "head"),
        P(("groups", "seq", "sub"), None, None, "head"),
        P("groups", None),
        P("groups"),
        P("groups"),
    )
    return jax.shard_map(
        per_device,
        mesh=mesh,
        in_specs=placed,
        out_specs=P(("groups", "seq"), None, "head"),
        check_vma=False,
    )
```

```python
import functools

import jax
import jax.numpy as jnp
from jax import lax
from jax.experimental import pallas as pl
from jax.experimental.pallas import tpu as pltpu
from jax.sharding import PartitionSpec as P

HD = 128
PAGE = 128


NEG_FILL = -1e30


def partial_softmax(
    query_heads, cache_keys, cache_values, cache_valid, fresh_keys, fresh_values, fresh_valid
):
    score_scale = HD ** (-0.5)
    cache_scores = (
        jnp.einsum("rkgd,nkd->kgrn", query_heads, cache_keys, preferred_element_type=jnp.float32)
        * score_scale
    )
    fresh_scores = (
        jnp.einsum("rkgd,jkd->kgrj", query_heads, fresh_keys, preferred_element_type=jnp.float32)
        * score_scale
    )
    cache_mask = cache_valid[None, None, None, :]
    fresh_mask = fresh_valid[None, None, :, :]
    peak = jnp.maximum(
        jnp.max(jnp.where(cache_mask, cache_scores, NEG_FILL), axis=-1),
        jnp.max(jnp.where(fresh_mask, fresh_scores, NEG_FILL), axis=-1),
    )
    cache_weights = jnp.where(cache_mask, jnp.exp(cache_scores - peak[..., None]), 0.0)
    fresh_weights = jnp.where(fresh_mask, jnp.exp(fresh_scores - peak[..., None]), 0.0)
    weight_sum = jnp.sum(cache_weights, axis=-1) + jnp.sum(fresh_weights, axis=-1)
    numerator = jnp.einsum(
        "kgrn,nkd->kgrd",
        cache_weights.astype(jnp.bfloat16),
        cache_values,
        preferred_element_type=jnp.float32,
    )
    numerator = numerator + jnp.einsum(
        "kgrj,jkd->kgrd",
        fresh_weights.astype(jnp.bfloat16),
        fresh_values,
        preferred_element_type=jnp.float32,
    )
    return (peak, weight_sum, numerator)


def attend_all(
    query_block, fresh_block, received, fetch_index, page_here, lengths, live_rows, causal, fresh_on
):
    kv_width = received.shape[-1]
    heads_kv = kv_width // HD
    row_count = query_block.shape[1]
    group_size = query_block.shape[2] // kv_width
    page_count = fetch_index.shape[1]
    positions = jnp.arange(page_count * PAGE, dtype=jnp.int32)

    def one_sequence(inputs):
        query_rows, fresh_rows, index_row, here_row, length, live_row = inputs
        fetched = jnp.take(received, index_row, axis=0)
        cache_keys = fetched[:, 0].reshape(page_count * PAGE, heads_kv, HD)
        cache_values = fetched[:, 1].reshape(page_count * PAGE, heads_kv, HD)
        page_mask = jnp.broadcast_to(here_row[:, None], (page_count, PAGE)).reshape(
            page_count * PAGE
        )
        cache_valid = page_mask & (positions < length)
        query_heads = query_rows.reshape(row_count, heads_kv, group_size, HD)
        fresh_keys = fresh_rows[:, 0].reshape(row_count, heads_kv, HD)
        fresh_values = fresh_rows[:, 1].reshape(row_count, heads_kv, HD)
        fresh_valid = causal & live_row[:, None] & fresh_on
        return partial_softmax(
            query_heads,
            cache_keys,
            cache_values,
            cache_valid,
            fresh_keys,
            fresh_values,
            fresh_valid,
        )

    return lax.map(
        one_sequence, (query_block, fresh_block, fetch_index, page_here, lengths, live_rows)
    )


def finish(weight_sum, numerator, live_rows):
    unused_rows = 1.0 - live_rows.astype(jnp.float32)
    attended = numerator / (weight_sum + unused_rows[:, None, None, :])[..., None]
    attended = jnp.where(live_rows[:, None, None, :, None], attended, 0.0)
    seq_dev, heads_kv, group_size, row_count, head_dim = attended.shape
    return (
        jnp.transpose(attended, (0, 3, 1, 2, 4))
        .reshape(seq_dev, row_count, heads_kv * group_size * head_dim)
        .astype(jnp.bfloat16)
    )


def exchange_pages(queries, new_kv, kv_pages, page_table, cached_len, is_prefill):
    seq_shards = lax.axis_size("seq")
    sub_count = lax.axis_size("sub")
    owners = seq_shards * sub_count
    seq_index = lax.axis_index("seq")
    core_index = lax.axis_index("sub")
    owner_self = seq_index * sub_count + core_index
    seq_dev, row_count, query_width = queries.shape
    pages_dev = kv_pages.shape[0]
    kv_width = kv_pages.shape[3]
    page_count = page_table.shape[1]
    entries = seq_dev * page_count
    capacity = (entries + owners - 1) // owners
    table_rows = page_table.reshape(seq_shards, entries)
    holder = jnp.where(table_rows >= 0, table_rows // pages_dev, -1)
    slot_of = jnp.where(table_rows >= 0, table_rows % pages_dev, 0)
    owned_here = holder == owner_self
    rank_among = jnp.cumsum(owned_here.astype(jnp.int32), axis=1) - 1
    picked = owned_here[:, :, None] & (
        rank_among[:, :, None] == jnp.arange(capacity, dtype=jnp.int32)[None, None, :]
    )
    send_slots = jnp.sum(jnp.where(picked, slot_of[:, :, None], 0), axis=1).reshape(
        seq_shards * capacity
    )
    first_seq = seq_index * seq_dev
    my_table = lax.dynamic_slice_in_dim(page_table, first_seq, seq_dev, 0)
    my_lengths = lax.dynamic_slice_in_dim(cached_len, first_seq, seq_dev, 0)
    my_flags = lax.dynamic_slice_in_dim(is_prefill, first_seq, seq_dev, 0)
    flat_table = my_table.reshape(entries)
    my_holder = jnp.where(flat_table >= 0, flat_table // pages_dev, -1)
    entry_order = jnp.arange(entries, dtype=jnp.int32)
    earlier = (my_holder[:, None] == my_holder[None, :]) & (
        entry_order[None, :] < entry_order[:, None]
    )
    my_rank = jnp.sum(earlier.astype(jnp.int32), axis=1)
    row_ids = jnp.arange(row_count, dtype=jnp.int32)
    live_rows = (my_flags[:, None] == 1) | (row_ids[None, :] == 0)
    causal = row_ids[None, :] <= row_ids[:, None]
    part_width = kv_width // sub_count
    split_pages = kv_pages.reshape(pages_dev, 2, PAGE, sub_count, part_width)
    chosen = jnp.take(split_pages, send_slots, axis=0).reshape(
        seq_shards, capacity, 2, PAGE, sub_count, part_width
    )
    outgoing = jnp.moveaxis(chosen, 4, 1).reshape(owners, capacity, 2, PAGE, part_width)
    received = lax.all_to_all(
        outgoing, ("seq", "sub"), split_axis=0, concat_axis=0, tiled=True
    ).reshape(owners * capacity, 2, PAGE, part_width)
    present = flat_table >= 0
    fetch_index = jnp.where(present, my_holder * capacity + my_rank, 0)
    query_part = query_width // sub_count
    my_queries = lax.dynamic_slice_in_dim(queries, core_index * query_part, query_part, 2)
    my_fresh = lax.dynamic_slice_in_dim(new_kv, core_index * part_width, part_width, 3)
    peak, weight_sum, numerator = attend_all(
        my_queries,
        my_fresh,
        received,
        fetch_index.reshape(seq_dev, page_count),
        present.reshape(seq_dev, page_count),
        my_lengths,
        live_rows,
        causal,
        core_index >= 0,
    )
    own_heads = finish(weight_sum, numerator, live_rows)
    return lax.all_gather(own_heads, "sub", axis=2, tiled=True)


MESH = pl.DeviceIdType.MESH
SCALE = HD ** (-0.5)
LOG2E = 1.4426950408889634


def greet(z, n):
    has_left, has_right = z > 0, z < n - 1
    barrier = pltpu.get_barrier_semaphore()

    @pl.when(has_left)
    def _():
        pl.semaphore_signal(barrier, inc=1, device_id={"seq": z - 1}, device_id_type=MESH)

    @pl.when(has_right)
    def _():
        pl.semaphore_signal(barrier, inc=1, device_id={"seq": z + 1}, device_id_type=MESH)

    pl.semaphore_wait(barrier, has_left.astype(jnp.int32) + has_right.astype(jnp.int32))
    return has_left, has_right


def remote(src, dst, send, recv, z):
    return pltpu.make_async_remote_copy(
        src_ref=src, dst_ref=dst, send_sem=send, recv_sem=recv,
        device_id={"seq": z}, device_id_type=MESH,
    )


DEC_MAXP = 4


def line_steps(z, n, count, lag, from_left, from_right, last):
    def guarded(c, work):
        @pl.when((c >= 0) & (c < count))
        def _():
            work(c)

    def step(s, carry):
        guarded(s - lag * z, from_left)
        guarded(s - lag * (n - 1 - z), from_right)
        guarded(s - lag * jnp.maximum(z, n - 1 - z), last)
        return carry

    lax.fori_loop(0, count + lag * (n - 1), step, 0)


def gather_queries_kernel(n, count, own, out, rin, rout, lin, lout, rs, rr, ls, lr):
    z = lax.axis_index("seq")
    has_left, has_right = greet(z, n)

    def right(c):
        return remote(rout.at[c], rin.at[c], rs.at[c], rr.at[c], z + 1)

    def left(c):
        return remote(lout.at[c], lin.at[c], ls.at[c], lr.at[c], z - 1)

    def from_left(c):
        @pl.when(has_left)
        def _():
            right(c).wait_recv()
            rout[c] = own[c] + rin[c]

        @pl.when(jnp.logical_not(has_left))
        def _():
            rout[c] = own[c]

        @pl.when(has_right)
        def _():
            right(c).start()

    def from_right(c):
        @pl.when(has_right)
        def _():
            left(c).wait_recv()
            lout[c] = own[c] + lin[c]

        @pl.when(jnp.logical_not(has_right))
        def _():
            lout[c] = own[c]

        @pl.when(has_left)
        def _():
            left(c).start()

    def last(c):
        @pl.when(has_right)
        def _():
            out[c] = rout[c] + lin[c]

        @pl.when(jnp.logical_not(has_right))
        def _():
            out[c] = rout[c]

    line_steps(z, n, count, 4, from_left, from_right, last)

    def drain(c, carry):
        @pl.when(has_right)
        def _():
            right(c).wait_send()

        @pl.when(has_left)
        def _():
            left(c).wait_send()

        return carry

    lax.fori_loop(0, count, drain, 0)


def gather_queries(own, n):
    total, width = own.shape
    rows = 16
    count = total // rows
    shape = (count, rows, width)
    buffer = pltpu.VMEM(shape, own.dtype)
    return pl.pallas_call(
        functools.partial(gather_queries_kernel, n, count),
        out_shape=jax.ShapeDtypeStruct(shape, own.dtype),
        in_specs=[pl.BlockSpec(memory_space=pltpu.VMEM)],
        out_specs=pl.BlockSpec(memory_space=pltpu.VMEM),
        scratch_shapes=[buffer] * 4 + [pltpu.SemaphoreType.DMA((count,))] * 4,
        compiler_params=pltpu.CompilerParams(collective_id=0, has_side_effects=True),
        name="gather_queries",
    )(own.reshape(shape)).reshape(total, width)


def merge(o1, e1, o2, e2):
    top = jnp.maximum(e1, e2)
    w1, w2 = jnp.exp(e1 - top), jnp.exp(e2 - top)
    total = w1 + w2
    inv = 1.0 / total
    return o1 * (w1 * inv) + o2 * (w2 * inv), top + jnp.log(total)


def reduce_outputs_kernel(
    n, count, o, e, out, oute, ri, ro, li, lo, rei, reo, lei, leo, rs, rr, ls, lr, res, rer, les, ler
):
    z = lax.axis_index("seq")
    has_left, has_right = greet(z, n)

    def right(c):
        return (
            remote(ro.at[c], ri.at[c], rs.at[c], rr.at[c], z + 1),
            remote(reo.at[c], rei.at[c], res.at[c], rer.at[c], z + 1),
        )

    def left(c):
        return (
            remote(lo.at[c], li.at[c], ls.at[c], lr.at[c], z - 1),
            remote(leo.at[c], lei.at[c], les.at[c], ler.at[c], z - 1),
        )

    def join(o1, e1, o2, e2, oo, eo, c):
        joined, stat = merge(o1[c].astype(jnp.float32), e1[c], o2[c].astype(jnp.float32), e2[c])
        oo[c] = joined.astype(oo.dtype)
        eo[c] = stat

    def from_left(c):
        @pl.when(has_left)
        def _():
            for x in right(c):
                x.wait_recv()
            join(o, e, ri, rei, ro, reo, c)

        @pl.when(jnp.logical_not(has_left))
        def _():
            ro[c] = o[c]
            reo[c] = e[c]

        @pl.when(has_right)
        def _():
            for x in right(c):
                x.start()

    def from_right(c):
        @pl.when(has_right)
        def _():
            for x in left(c):
                x.wait_recv()
            join(o, e, li, lei, lo, leo, c)

        @pl.when(jnp.logical_not(has_right))
        def _():
            lo[c] = o[c]
            leo[c] = e[c]

        @pl.when(has_left)
        def _():
            for x in left(c):
                x.start()

    def last(c):
        @pl.when(has_right)
        def _():
            join(ro, reo, li, lei, out, oute, c)

        @pl.when(jnp.logical_not(has_right))
        def _():
            out[c] = ro[c]
            oute[c] = reo[c]

    line_steps(z, n, count, 2, from_left, from_right, last)

    def drain(c, carry):
        @pl.when(has_right)
        def _():
            for x in right(c):
                x.wait_send()

        @pl.when(has_left)
        def _():
            for x in left(c):
                x.wait_send()

        return carry

    lax.fori_loop(0, count, drain, 0)


def reduce_outputs(o, e, n):
    count = e.shape[0]
    return pl.pallas_call(
        functools.partial(reduce_outputs_kernel, n, count),
        out_shape=[jax.ShapeDtypeStruct(x.shape, x.dtype) for x in (o, e)],
        in_specs=[pl.BlockSpec(memory_space=pltpu.VMEM)] * 2,
        out_specs=[pl.BlockSpec(memory_space=pltpu.VMEM)] * 2,
        scratch_shapes=[pltpu.VMEM(o.shape, o.dtype)] * 4
        + [pltpu.VMEM(e.shape, e.dtype)] * 4
        + [pltpu.SemaphoreType.DMA((count,))] * 8,
        compiler_params=pltpu.CompilerParams(collective_id=1, has_side_effects=True),
        name="reduce_outputs",
    )(o, e)[0]


def stacked_heads(rows, k, group_size):
    return jnp.concatenate(
        [rows[:, (k * group_size + g) * HD : (k * group_size + g + 1) * HD] for g in range(group_size)], axis=0
    )


def scores_of(keys, query):
    return lax.dot_general(keys, query, (((1,), (1,)), ((), ())), preferred_element_type=jnp.float32)


def partial_outputs(query, blocks):
    scored = [jnp.where(mask, scores_of(keys, query), NEG_FILL) for keys, _, mask in blocks]
    peak = functools.reduce(jnp.maximum, [jnp.max(s, axis=0, keepdims=True) for s in scored])
    peak = jnp.maximum(peak, 0.1 * NEG_FILL)
    acc, total = None, None
    for s, (_, values, _) in zip(scored, blocks):
        weights = jnp.exp2((s - peak) * (SCALE * LOG2E))
        part = jnp.sum(weights, axis=0, keepdims=True)
        prod = lax.dot_general(
            values, weights.astype(jnp.bfloat16), (((0,), (0,)), ((), ())), preferred_element_type=jnp.float32
        )
        acc = prod if acc is None else acc + prod
        total = part if total is None else total + part
    empty = total == 0.0
    total = jnp.where(empty, 1.0, total)
    return acc * (1.0 / total), jnp.where(empty, NEG_FILL, peak * SCALE + jnp.log(total))


def prefill_kernel(most, heads, group_size, pages, valid, home, local, q_ref, *refs):
    page_refs, (fk_ref, fv_ref, o_ref, e_ref) = refs[:most], refs[most:]
    j = pl.program_id(0)
    rows = q_ref.shape[0]
    lanes = group_size * rows
    key_id = lax.broadcasted_iota(jnp.int32, (PAGE, 1), 0)
    fresh_id = lax.broadcasted_iota(jnp.int32, (rows, lanes), 0)
    lane_row = lax.broadcasted_iota(jnp.int32, (rows, lanes), 1) % rows
    for k in range(heads):
        cols = slice(k * HD, (k + 1) * HD)
        query = stacked_heads(q_ref, k, group_size)
        blocks = [
            (ref[0, 0, :, cols], ref[0, 1, :, cols], key_id < valid[j, i]) for i, ref in enumerate(page_refs)
        ]
        fresh_mask = (fresh_id <= lane_row) & (home[j] == 1)
        blocks.append((fk_ref[0, :, cols], fv_ref[0, :, cols], fresh_mask))
        o, e = partial_outputs(query, blocks)
        o_ref[k] = o.astype(o_ref.dtype)
        e_ref[k] = e


def decode_kernel(columns, heads, group_size, seqs, pages, valid, home, local, seq, q_ref, *refs):
    page_refs, (fk_ref, fv_ref, _, _, o_ref, e_ref) = refs[: len(columns)], refs[len(columns) :]
    j = pl.program_id(0)
    lanes = group_size * seqs
    fresh_rows = 16
    key_id = lax.broadcasted_iota(jnp.int32, (PAGE, 1), 0)
    fresh_id = lax.broadcasted_iota(jnp.int32, (fresh_rows, 1), 0)
    mine = lax.broadcasted_iota(jnp.int32, (1, lanes), 1) % seqs == seq[j]

    @pl.when(j == 0)
    def _():
        o_ref[...] = jnp.zeros_like(o_ref)
        e_ref[...] = jnp.full_like(e_ref, NEG_FILL)

    for k in range(heads):
        cols = slice(k * HD, (k + 1) * HD)
        query = stacked_heads(q_ref, k, group_size)
        blocks = [
            (ref[0, 0, :, cols], ref[0, 1, :, cols], key_id < valid[j, i]) for i, ref in zip(columns, page_refs)
        ]
        fresh_mask = fresh_id < home[j]
        blocks.append((fk_ref[0, :fresh_rows, cols], fv_ref[0, :fresh_rows, cols], fresh_mask))
        o, e = partial_outputs(query, blocks)
        place = slice(k * lanes, (k + 1) * lanes)
        o_ref[0, :, place] = jnp.where(mine, o, o_ref[0, :, place].astype(jnp.float32)).astype(o_ref.dtype)
        e_ref[0, :, place] = jnp.where(mine, e, e_ref[0, :, place])


def finish_kernel(heads, group_size, seqs, slot, flag, first, o_ref, od_ref, out_ref):
    i = pl.program_id(0)
    rows = out_ref.shape[1]

    @pl.when(flag[i] == 1)
    def _():
        for k in range(heads):
            turned = o_ref[k].astype(jnp.float32).T.astype(out_ref.dtype)
            for g in range(group_size):
                h = k * group_size + g
                out_ref[0, :, h * HD : (h + 1) * HD] = turned[g * rows : (g + 1) * rows]

    @pl.when(flag[i] != 1)
    def _():
        top = lax.broadcasted_iota(jnp.int32, (rows, 1), 0) == 0
        pick = lax.broadcasted_iota(jnp.int32, (seqs, 1), 0) == first[0] + i
        for k in range(heads):
            place = slice(k * seqs * group_size, (k + 1) * seqs * group_size)
            turned = od_ref[0, :, place].astype(jnp.float32).T
            for g in range(group_size):
                h = k * group_size + g
                line = jnp.sum(jnp.where(pick, turned[g * seqs : (g + 1) * seqs], 0.0), axis=0, keepdims=True)
                out_ref[0, :, h * HD : (h + 1) * HD] = jnp.where(top, line, 0.0).astype(out_ref.dtype)


def move_queries(queries, new_kv, kv_pages, page_table, cached_len, is_prefill):
    n = lax.axis_size("seq")
    sub_count = lax.axis_size("sub")
    z = lax.axis_index("seq")
    core = lax.axis_index("sub")
    seq_dev, row_count, query_width = queries.shape
    pages_dev, kv_width = kv_pages.shape[0], kv_pages.shape[3]
    seqs, page_count = page_table.shape
    owners = n * sub_count
    each = page_count // owners
    most = sub_count * each
    slots = seqs // 2
    group_size = query_width // kv_width
    part_width, query_part = kv_width // sub_count, query_width // sub_count
    heads = part_width // HD

    other = (core + 1) % sub_count
    away = lax.dynamic_slice_in_dim(kv_pages, other * part_width, part_width, 3)
    came = lax.ppermute(away, "sub", [(c, (c + 1) % sub_count) for c in range(sub_count)])

    seq_ids = jnp.arange(seqs, dtype=jnp.int32)
    owner = jnp.where(page_table >= 0, page_table // pages_dev, -1)
    sources = z * sub_count + jnp.stack([core, other])
    mine = owner[None] == sources[:, None, None]
    rank = jnp.cumsum(mine.astype(jnp.int32), axis=2) - 1
    picked = mine[..., None] & (rank[..., None] == jnp.arange(each, dtype=jnp.int32))
    tokens = jnp.clip(cached_len[:, None] - PAGE * jnp.arange(page_count, dtype=jnp.int32), 0, PAGE)

    def listed(values):
        found = jnp.sum(jnp.where(picked, values[None, :, :, None], 0), axis=2)
        return jnp.moveaxis(found, 0, 1).reshape(seqs, most)

    page_rows, valid_rows = listed(page_table % pages_dev), listed(tokens)
    flags = is_prefill == 1
    slot_of = jnp.cumsum(flags.astype(jnp.int32)) - 1
    place_of = jnp.cumsum((~flags).astype(jnp.int32)) - 1
    slot_ids = jnp.arange(slots, dtype=jnp.int32)
    slot_seq = jnp.sum(jnp.where(flags & (slot_of == slot_ids[:, None]), seq_ids, 0), axis=1)
    rest_ids = jnp.arange(seqs - slots, dtype=jnp.int32)
    rest_seq = jnp.sum(jnp.where(~flags & (place_of == rest_ids[:, None]), seq_ids, 0), axis=1)

    def tables(which):
        at_home = (which // seq_dev == z).astype(jnp.int32)
        places = jnp.where(at_home == 1, which % seq_dev, 0)
        chosen = which[:, None, None] == seq_ids[None, :, None]
        rows = [jnp.sum(jnp.where(chosen, x[None], 0), axis=1) for x in (page_rows, valid_rows)]
        return rows[0], rows[1], at_home, jnp.append(places, core)

    slot_tables, rest_tables = tables(slot_seq), tables(rest_seq)
    my_queries = lax.dynamic_slice_in_dim(queries, core * query_part, query_part, 2)
    own_slots = jnp.where((slot_tables[2] == 1)[:, None, None], my_queries[slot_tables[3][:slots]], 0)
    first_rows = jnp.where(
        (seq_ids // seq_dev == z)[:, None], jnp.tile(my_queries[:, 0], (n, 1)), 0
    )
    own = jnp.concatenate([own_slots.reshape(slots * row_count, query_part), first_rows], axis=0)
    gathered = gather_queries(own.astype(queries.dtype), n)

    my_fresh = lax.dynamic_slice_in_dim(new_kv, core * part_width, part_width, 3)
    fresh_keys, fresh_values = my_fresh[:, :, 0], my_fresh[:, :, 1]
    lanes = group_size * row_count
    count = slots * heads + 1

    def page_spec(i):
        if i >= each:
            return pl.BlockSpec((1, 2, PAGE, part_width), lambda j, pages, *_: (pages[j, i], 0, 0, 0))
        return pl.BlockSpec(
            (1, 2, PAGE, part_width),
            lambda j, pages, valid, home, local, *_: (pages[j, i], 0, 0, local[local.shape[0] - 1]),
        )

    fresh_spec = pl.BlockSpec(
        (1, row_count, part_width), lambda j, pages, valid, home, local, *_: (local[j], 0, 0)
    )
    o, e = pl.pallas_call(
        functools.partial(prefill_kernel, most, heads, group_size),
        grid_spec=pltpu.PrefetchScalarGridSpec(
            num_scalar_prefetch=4,
            grid=(slots,),
            in_specs=[pl.BlockSpec((row_count, query_part), lambda j, *_: (j, 0))]
            + [page_spec(i) for i in range(most)]
            + [fresh_spec] * 2,
            out_specs=[
                pl.BlockSpec((heads, HD, lanes), lambda j, *_: (j, 0, 0)),
                pl.BlockSpec((heads, 1, lanes), lambda j, *_: (j, 0, 0)),
            ],
        ),
        out_shape=[
            jax.ShapeDtypeStruct((count, HD, lanes), jnp.bfloat16),
            jax.ShapeDtypeStruct((count, 1, lanes), jnp.float32),
        ],
        name="prefill_attention",
    )(*slot_tables, gathered, *([kv_pages] * each), *([came] * (most - each)), fresh_keys, fresh_values)
    few = min(each, -(-DEC_MAXP // owners))
    columns = [*range(few), *range(each, each + few)]
    o, e = pl.pallas_call(
        functools.partial(decode_kernel, columns, heads, group_size, seqs),
        grid_spec=pltpu.PrefetchScalarGridSpec(
            num_scalar_prefetch=5,
            grid=(seqs - slots,),
            in_specs=[pl.BlockSpec((seqs, query_part), lambda j, *_: (slots * row_count // seqs, 0))]
            + [page_spec(i) for i in columns]
            + [fresh_spec] * 2
            + [pl.BlockSpec(memory_space=pl.ANY)] * 2,
            out_specs=[
                pl.BlockSpec((1, HD, lanes), lambda j, *_: (count - 1, 0, 0)),
                pl.BlockSpec((1, 1, lanes), lambda j, *_: (count - 1, 0, 0)),
            ],
        ),
        out_shape=[jax.ShapeDtypeStruct(x.shape, x.dtype) for x in (o, e)],
        input_output_aliases={8 + len(columns): 0, 9 + len(columns): 1},
        name="decode_attention",
    )(*rest_tables, rest_seq, gathered, *([kv_pages] * few), *([came] * few), fresh_keys, fresh_values, o, e)
    o = reduce_outputs(o, e, n)

    first_seq = z * seq_dev
    my_flags = lax.dynamic_slice_in_dim(is_prefill, first_seq, seq_dev, 0)
    my_slots = jnp.maximum(lax.dynamic_slice_in_dim(slot_of, first_seq, seq_dev, 0), 0)
    own_heads = pl.pallas_call(
        functools.partial(finish_kernel, heads, group_size, seqs),
        grid_spec=pltpu.PrefetchScalarGridSpec(
            num_scalar_prefetch=3,
            grid=(seq_dev,),
            in_specs=[
                pl.BlockSpec((heads, HD, lanes), lambda i, slot, *_: (slot[i], 0, 0)),
                pl.BlockSpec((1, HD, lanes), lambda i, *_: (count - 1, 0, 0)),
            ],
            out_specs=pl.BlockSpec((1, row_count, query_part), lambda i, *_: (i, 0, 0)),
        ),
        out_shape=jax.ShapeDtypeStruct((seq_dev, row_count, query_part), jnp.bfloat16),
        name="finish",
    )(my_slots, my_flags, jnp.reshape(first_seq, (1,)).astype(jnp.int32), o, o)
    pairs = [(c, (c + 1) % sub_count) for c in range(sub_count)]
    came_heads = lax.ppermute(own_heads, "sub", pairs)
    first_half = jnp.where(core == 0, own_heads, came_heads)
    second_half = jnp.where(core == 0, came_heads, own_heads)
    return jnp.concatenate([first_half, second_half], axis=2)


def per_device(queries, new_kv, kv_pages, page_table, cached_len, is_prefill):
    owners = lax.axis_size("seq") * lax.axis_size("sub")
    if page_table.shape[1] >= owners:
        return move_queries(queries, new_kv, kv_pages, page_table, cached_len, is_prefill)
    return exchange_pages(queries, new_kv, kv_pages, page_table, cached_len, is_prefill)


def solution(mesh):
    placed = (
        P(("groups", "seq"), None, "head"),
        P(("groups", "seq"), None, None, "head"),
        P(("groups", "seq", "sub"), None, None, "head"),
        P("groups", None),
        P("groups"),
        P("groups"),
    )
    return jax.shard_map(
        per_device,
        mesh=mesh,
        in_specs=placed,
        out_specs=P(("groups", "seq"), None, "head"),
        check_vma=False,
    )
```
